256 devices in a mesh: grp: 2 (over core), gx: 32 (over z, x), gy: 4 (over y).
Axes of the slice: x: 4, y: 4, z: 8, core: 2. Of those that a mesh axis runs over, the one named last changes fastest.
Arguments:
- fields: float32 [2, 3, 1024, 512], P('grp', None, 'gx', 'gy'), may hold values from -6 to 6
- coefficients: float32 [2, 1024, 512], P('grp', 'gx', 'gy'), may hold values from 0.05 to 0.24
- forcing: float32 [2, 3, 1024, 512], P('grp', None, 'gx', 'gy'), may hold values from -4 to 4
- element_matrix: float32 [12, 12], replicated, as said below
- source_cells: int32 [2, 8192, 128], P('grp', ('gx', 'gy')), may hold values from 0 to 4095
- target_cells: int32 [2, 8192, 128], P('grp', ('gx', 'gy')), may hold values from 0 to 4095
- peer_map: int32 [2, 8192, 1], P('grp', ('gx', 'gy')), may hold values from 0 to 127; in each aligned block of 64 rows (0 to 63, 64 to 127, ..., all dimensions but the last counted through in order) at most 2 rows name the same one
- mapping_blocks: bfloat16 [2, 8192, 128, 128], P('grp', ('gx', 'gy')), may hold values from -0.25 to 0.25
Outputs:
- new_fields: float32 [2, 3, 1024, 512], P('grp', None, 'gx', 'gy')
- interface_load: float32 [2, 3, 1024, 512], P('grp', None, 'gx', 'gy')
The draws below stay inside these ranges and needn't reach their ends.
Inputs may be any that keep to these rules, and one draw needn't show every extreme that they name: `peer_map`: within the 64 blocks of one partition no receiving partition is named more than 2 times. `source_cells`: local point indices of the sending partition. `target_cells`: local point indices of the receiving partition. `element_matrix`: Symmetric; every diagonal entry exceeds the sum of magnitudes of the other entries of its row by 0.5 or more.
All inputs are finite; a program needn't handle non-finite values.
Results may differ from the reference program's by a relative error of at most 0.012.
Values sent between devices are 32-bit elements; how exact they have to be, the bound alone decides.
No kernel may reach another device: no remote copies, remote signals or barrier semaphores. Data moves between devices by JAX's collectives and lax.ppermute only.
A program may use at most 128 MiB of HBM per device.

```python
import math
import jax
import jax.numpy as jnp
import numpy as np
from jax import lax

CX = 32
CY = 128
NBLK = 64
BLOCK = 128
ITERS = 4
SUB = 4
PARTS_SIZE = 128
CAP = 2
NX = 1024
NY = 512
N_GX = 32
N_GY = 4


def draw_element_matrix(key, part):
    first, second = jax.random.split(jax.random.fold_in(key, 11))
    rough = jax.random.normal(first, (12, 12), jnp.float32) * 0.25
    symmetric = 0.5 * (rough + rough.T)
    offdiag = symmetric * (1.0 - jnp.eye(12, dtype=jnp.float32))
    margin = jax.random.uniform(second, (12,), jnp.float32, 0.5, 1.5)
    return offdiag + jnp.diag(jnp.sum(jnp.abs(offdiag), axis=1) + margin)


def touch_ends(result, key, low, top_value):
    longest = result.shape.index(max(result.shape))
    spots = []
    for shift in (0, 1):
        where = [jax.random.randint(jax.random.fold_in(key, axis), (), 0, length) for axis, length in enumerate(result.shape)]
        where[longest] = (where[longest] + shift) % result.shape[longest]
        spots.append(tuple(where))
    return result.at[spots[0]].set(low).at[spots[1]].set(top_value)


def steps_of(stream_key, dims, cuts, smallest, largest):
    factor_of, own = 1.0, jax.random.fold_in(stream_key, 6)
    for axis_at, parts in cuts:
        heights = jnp.exp(jax.random.uniform(jax.random.fold_in(own, axis_at), (parts,), jnp.float32, smallest / len(cuts), largest / len(cuts)))
        factor_of = factor_of * jnp.repeat(heights, dims[axis_at] // parts).reshape([-1 if axis == axis_at else 1 for axis in range(len(dims))])
    return factor_of


def deal_out(own_key, own, number, rows, count, top, most, skew):
    ranking = jax.random.permutation(own_key, count)
    crowded, ordinary = shares(count, rows * top, most, skew, True), shares(count, rows * top, most, skew, False)
    places = jnp.arange(count)

    def named(sizes, turn):
        used = int((sizes > 0).sum())
        fixed = max(1, used // 4)
        passed = fixed + (places - fixed + turn * (used - fixed)) % max(1, count - fixed)
        return jnp.zeros((count,), jnp.int32).at[ranking[jnp.where(places < fixed, places, passed)]].set(jnp.asarray(sizes, jnp.int32))

    sizes = jnp.where(number % 4 == 0, named(crowded, number // 4), named(ordinary, number - number // 4 - 1))
    mixed = jax.random.permutation(jax.random.fold_in(own, 3), count)
    source_of, receiver = mixed[0:count // 2 * 2:2], mixed[1:count // 2 * 2:2]
    room = jnp.minimum(sizes[source_of] - 1, most - sizes[receiver]) // 2
    room = jnp.where((source_of == ranking[0]) | (receiver == ranking[0]) | (sizes[receiver] == 0), 0, jnp.maximum(room, 0))
    passed = jax.random.randint(jax.random.fold_in(own, 4), (count // 2,), 0, 1 << 20) % (room + 1)
    sizes = sizes.at[source_of].add(-passed).at[receiver].add(passed)
    items = jnp.searchsorted(jnp.cumsum(sizes), jnp.arange(rows * top), side="right").astype(jnp.int32)
    grid = items.reshape(top, rows).T
    grid = grid[jax.random.permutation(jax.random.fold_in(own, 1), rows)]
    turn = jax.random.randint(jax.random.fold_in(own, 2), (rows, 1), 0, top)
    return jnp.take_along_axis(grid, (jnp.arange(top)[None, :] + turn) % top, axis=1)


def shares(amount, total, reach, skew, full):
    loads = [(1 << 20) // math.isqrt(rank ** skew) + 1 for rank in range(1, amount + 1)]
    largest = reach if full else min(reach, max(-(-total // amount), total * loads[0] // sum(loads)))
    least = 1 if total - largest >= amount - 1 else 0
    counts, spare = [largest] + [least] * (amount - 1), total - largest - least * (amount - 1)
    while spare > 0:
        free = [i for i in range(1, amount) if counts[i] < largest] or [i for i in range(1, amount) if counts[i] < reach]
        mass, left = sum([loads[i] for i in free]), spare
        for i in free:
            addition = min(reach - counts[i], max(1, left * loads[i] // mass), spare)
            counts[i] = counts[i] + addition
            spare = spare - addition
    return np.array(counts)


def noise(stream_key, extent, deviation, limit, cuts=(), kind=jnp.bfloat16):
    factor_of = steps_of(stream_key, extent, cuts, -0.22, 0.18) if cuts else 1.0
    values = jax.random.normal(stream_key, extent, jnp.float32) * deviation * factor_of
    return jnp.minimum(jnp.maximum(values, -limit), limit).astype(kind)


def setup_inputs(seed: int = 0) -> dict:
    key_of = jax.random.split(jax.random.key(seed), 9)
    fields = noise(key_of[0], (2, 3, NX, NY), 1.0, 6.0, ((0, 2), (2, 32), (3, 4)), jnp.float32)
    coefficients = jnp.clip(jnp.exp(math.log(0.24) - 1.5686159 * jax.random.uniform(key_of[1], (2, NX, NY), jnp.float32) ** steps_of(key_of[1], (2, NX, NY), ((0, 2), (1, 32), (2, 4)), -0.2, 0.2)), 0.05, 0.24)
    forcing = noise(key_of[2], (2, 3, NX, NY), 0.3, 4.0, ((0, 2), (2, 32), (3, 4)), jnp.float32)
    element_matrix = draw_element_matrix(jax.random.fold_in(key_of[8], 71), 0)
    source_cells = touch_ends(jax.random.randint(key_of[4], (2, PARTS_SIZE * NBLK, BLOCK), 0, CX * CY), jax.random.fold_in(key_of[4], 1), 0, (CX * CY) - 1).astype(jnp.int32)
    target_cells = touch_ends(jax.random.randint(key_of[5], (2, PARTS_SIZE * NBLK, BLOCK), 0, CX * CY), jax.random.fold_in(key_of[5], 1), 0, (CX * CY) - 1).astype(jnp.int32)
    peer_map_keys = jax.random.split(jax.random.fold_in(key_of[6], 1), 2 * (PARTS_SIZE * NBLK) // NBLK)
    peer_map_turns = jax.random.permutation(jax.random.fold_in(key_of[6], 3), 2 * (PARTS_SIZE * NBLK) // NBLK)
    peer_map = jax.vmap(lambda own, number: deal_out(jax.random.fold_in(key_of[6], 2), own, number, NBLK, N_GX * N_GY, 1, CAP, 2))(peer_map_keys, peer_map_turns).reshape((2, PARTS_SIZE * NBLK, 1))
    mapping_blocks = noise(key_of[7], (2, PARTS_SIZE * NBLK, BLOCK, BLOCK), (4 * BLOCK) ** -0.5, 0.25, ((0, 2), (1, 128)))
    return dict(fields=fields, coefficients=coefficients, forcing=forcing, element_matrix=element_matrix, source_cells=source_cells, target_cells=target_cells, peer_map=peer_map, mapping_blocks=mapping_blocks)


DT_STEP = 1.0
RELAX = 0.6


def fluid_sweep(padded, viscous, forcing, applied):
    centre = padded[:, 1:-1, 1:-1]
    middle = viscous[1:-1, 1:-1]
    flux_sum = 0.5 * (middle + viscous[2:, 1:-1]) * (padded[:, 2:, 1:-1] - centre)
    flux_sum = flux_sum + 0.5 * (middle + viscous[:-2, 1:-1]) * (padded[:, :-2, 1:-1] - centre)
    flux_sum = flux_sum + 0.5 * (middle + viscous[1:-1, 2:]) * (padded[:, 1:-1, 2:] - centre)
    flux_sum = flux_sum + 0.5 * (middle + viscous[1:-1, :-2]) * (padded[:, 1:-1, :-2] - centre)
    return centre + DT_STEP * (flux_sum + forcing + applied)


def shell_sweep(padded, stiff_pad, element_matrix, forcing, applied):
    stiffness = stiff_pad[:-1, :-1]
    nodal = jnp.concatenate([padded[:, :-1, :-1], padded[:, 1:, :-1], padded[:, :-1, 1:], padded[:, 1:, 1:]], axis=0)
    element_force = jnp.einsum("ab,bxy->axy", element_matrix, nodal, precision=lax.Precision.HIGHEST) * stiffness
    nodal_force = element_force[0:3, 1:, 1:] + element_force[3:6, :-1, 1:]
    nodal_force = nodal_force + element_force[6:9, 1:, :-1] + element_force[9:12, :-1, :-1]
    diag_terms = jnp.diagonal(element_matrix)
    diagonal = diag_terms[0:3, None, None] * stiffness[None, 1:, 1:] + diag_terms[3:6, None, None] * stiffness[None, :-1, 1:]
    diagonal = diagonal + diag_terms[6:9, None, None] * stiffness[None, 1:, :-1] + diag_terms[9:12, None, None] * stiffness[None, :-1, :-1]
    return padded[:, 1:-1, 1:-1] + RELAX * (forcing + applied - nodal_force) / diagonal


def blocks_of(values):
    comps = values.shape[0]
    shaped = values.reshape(comps, N_GX, CX, N_GY, CY).transpose(1, 3, 0, 2, 4)
    return shaped.reshape(N_GX * N_GY, comps, CX * CY)


def grid_of(blocks):
    comps = blocks.shape[1]
    shaped = blocks.reshape(N_GX, N_GY, comps, CX, CY).transpose(2, 0, 3, 1, 4)
    return shaped.reshape(comps, CX * N_GX, CY * N_GY)


def outgoing(values, source_cells, mapping_blocks):
    partitions = N_GX * N_GY
    parted = blocks_of(values)

    def per_part(pieces):
        local, cells, matrices = pieces
        read = local[:, cells].astype(jnp.bfloat16).astype(jnp.float32)
        return jnp.einsum("cln,lnm->lcm", read, matrices.astype(jnp.float32))

    mapped = lax.map(per_part, (parted, source_cells.reshape(partitions, NBLK, BLOCK), mapping_blocks.reshape(partitions, NBLK, BLOCK, BLOCK)))
    return mapped.reshape(partitions * NBLK, 3, BLOCK)


def incoming(mapped, peer_map, target_cells):
    partitions = N_GX * N_GY
    where = (peer_map[:, 0:1] * (CX * CY) + target_cells).astype(jnp.int32)
    flat = jnp.zeros((3, partitions * CX * CY), jnp.float32)
    flat = flat.at[:, where.reshape(-1)].add(mapped.transpose(1, 0, 2).reshape(3, -1))
    return grid_of(flat.reshape(3, partitions, CX * CY).transpose(1, 0, 2))


def reference(fields, coefficients, forcing, element_matrix, source_cells, target_cells, peer_map, mapping_blocks):
    fluid_field = fields[0]
    shell_field = fields[1]
    viscous = jnp.pad(coefficients[0], 1)
    stiff_pad = jnp.pad(coefficients[1], 1)
    applied = jnp.zeros((2, 3, CX * N_GX, CY * N_GY), jnp.float32)
    edges = ((0, 0), (1, 1), (1, 1))
    for outer in range(ITERS):
        for inner in range(SUB):
            fluid_field = fluid_sweep(jnp.pad(fluid_field, edges), viscous, forcing[0], applied[0])
            shell_field = shell_sweep(jnp.pad(shell_field, edges), stiff_pad, element_matrix, forcing[1], applied[1])
        to_shell = incoming(outgoing(fluid_field, source_cells[0], mapping_blocks[0]), peer_map[0], target_cells[0])
        to_fluid = incoming(outgoing(shell_field, source_cells[1], mapping_blocks[1]), peer_map[1], target_cells[1])
        applied = jnp.stack([to_fluid, to_shell])
    return jnp.stack([fluid_field, shell_field]), applied
```

```python
import jax
import jax.numpy as jnp
from jax import lax
from jax.experimental import pallas as pl
from jax.experimental.pallas import tpu as pltpu
from jax.sharding import PartitionSpec as P

ITERS = 4
SUB = 4
HALO = 4
DT_STEP = 1.0
RELAX = 0.6
SLOT_ROWS = 4
CAPACITY = 2

INTERPRET = False

VMEM_SPEC = pl.BlockSpec(memory_space=pltpu.VMEM)
SMEM_SPEC = pl.BlockSpec(memory_space=pltpu.SMEM)
ANY_SPEC = pl.BlockSpec(memory_space=pl.ANY)


def lanes_of(shape):
    return lax.broadcasted_iota(jnp.int32, shape, len(shape) - 1)


def below(x):
    return pltpu.roll(x, x.shape[0] - 1, 0)


def above(x):
    return pltpu.roll(x, 1, 0)


def right(x):
    return pltpu.roll(x, x.shape[1] - 1, 1)


def left(x):
    return pltpu.roll(x, 1, 1)


def pack_sides(parts, left_out, right_out, top_out, bottom_out):
    rows, cols = parts[0].shape
    lane = lanes_of((rows, cols))
    low = jnp.zeros((rows, cols), jnp.float32)
    high = low
    for k, x in enumerate(parts):
        here = (lane >= HALO * k) & (lane < HALO * (k + 1))
        low = jnp.where(here, pltpu.roll(x, HALO * k, 1) if k else x, low)
        high = jnp.where(here, pltpu.roll(x, HALO * (k + 1), 1), high)
        top_out[HALO * k : HALO * (k + 1), :] = x[:HALO]
        bottom_out[HALO * k : HALO * (k + 1), :] = x[rows - HALO :]
    left_out[...] = low
    right_out[...] = high


def first_pack_kernel(coef_ref, force_ref, field_ref, left_out, right_out, top_out, bottom_out):
    parts = [coef_ref[...]] + [force_ref[c] for c in range(3)] + [field_ref[c] for c in range(3)]
    pack_sides(parts, left_out, right_out, top_out, bottom_out)


def pack_shapes(count, rows, cols):
    side = jax.ShapeDtypeStruct((rows, cols), jnp.float32)
    ends = jax.ShapeDtypeStruct((HALO * count, cols), jnp.float32)
    return [side, side, ends, ends]


def exchange(packed):
    low, high, top, bottom = packed
    count_x, count_y = lax.axis_size("gx"), lax.axis_size("gy")
    up_y = [(i, (i + 1) % count_y) for i in range(count_y)]
    down_y = [(j, i) for i, j in up_y]
    up_x = [(i, (i + 1) % count_x) for i in range(count_x)]
    down_x = [(j, i) for i, j in up_x]
    from_left = lax.ppermute(high, "gy", up_y)
    from_right = lax.ppermute(low, "gy", down_y)
    rows = low.shape[0]
    to_up = jnp.concatenate([top, from_left[:HALO], from_right[:HALO]], axis=0)
    to_down = jnp.concatenate([bottom, from_left[rows - HALO :], from_right[rows - HALO :]], axis=0)
    from_up = lax.ppermute(to_down, "gx", up_x)
    from_down = lax.ppermute(to_up, "gx", down_x)
    return from_left, from_right, from_up, from_down


def sweep_kernel(*refs, first, sizes, count_x, count_y):
    rows, cols, blocks = sizes
    tall, wide = rows + 2 * HALO, 2 * cols
    place_ref, slot_ref, elem_ref = refs[:3]
    if first:
        coef_ref, force_ref, field_ref = refs[3:6]
    else:
        static_ref, field_ref, applied_ref = refs[3:6]
    left_ref, right_ref, up_ref, down_ref, source_ref, target_ref, map_hbm = refs[6:13]
    outs = refs[13:]
    if first:
        state_out, send_out, static_out = outs[:3]
        scratch = outs[3:]
    else:
        state_out, send_out = outs[:2]
        scratch = outs[2:]
    ext, side_left, side_right, node, table, map_ref, map_sem = scratch
    fetch = pltpu.make_async_copy(map_hbm, map_ref, map_sem)
    fetch.start()
    send_out[...] = jnp.zeros(send_out.shape, jnp.float32)

    grp, place_x, place_y = place_ref[0], place_ref[1], place_ref[2]
    row_id = lax.broadcasted_iota(jnp.int32, (tall, wide), 0)
    col_id = lax.broadcasted_iota(jnp.int32, (tall, wide), 1)
    row_at = jnp.where(row_id < rows + HALO, row_id, row_id - tall) + place_x * rows
    col_in = jnp.where(col_id < cols + HALO, col_id, col_id - wide)
    col_at = col_in + place_y * cols
    keep = (row_at >= 0) & (row_at < rows * count_x) & (col_at >= 0) & (col_at < cols * count_y)
    keep = keep & (col_in >= -HALO)

    own = (
        [coef_ref[...]] + [force_ref[c] for c in range(3)] + [field_ref[c] for c in range(3)]
        if first
        else [field_ref[c] for c in range(3)] + [applied_ref[c] for c in range(3)]
    )
    count = len(own)
    base = HALO * count
    side_left[0:rows, :] = left_ref[...]
    side_left[rows : rows + HALO, :] = down_ref[base : base + HALO, :]
    side_left[rows + HALO : tall, :] = up_ref[base : base + HALO, :]
    side_right[0:rows, :] = right_ref[...]
    side_right[rows : rows + HALO, :] = down_ref[base + HALO : base + 2 * HALO, :]
    side_right[rows + HALO : tall, :] = up_ref[base + HALO : base + 2 * HALO, :]
    lane = lanes_of((tall, cols))
    for k in range(count):
        ext[k, 0:rows, 0:cols] = own[k]
        ext[k, rows : rows + HALO, 0:cols] = down_ref[HALO * k : HALO * (k + 1), :]
        ext[k, rows + HALO : tall, 0:cols] = up_ref[HALO * k : HALO * (k + 1), :]
        near = side_right[...]
        near = pltpu.roll(near, cols - HALO * k, 1) if k else near
        far = pltpu.roll(side_left[...], cols - HALO * (k + 1), 1)
        ext[k, :, cols:wide] = jnp.where(lane < HALO, near, far)
        ext[k] = jnp.where(keep, ext[k], 0.0)
    if first:
        for k in range(4):
            static_out[k] = ext[k]
        at = 4
    else:
        at = 0

    def static(k):
        return ext[k] if first else static_ref[k]

    def load(c):
        return static(1 + c) if first else static(1 + c) + ext[3 + c]

    @pl.when(grp == 0)
    def _():
        nu = static(0)
        weights = [0.5 * (nu + move(nu)) for move in (below, above, right, left)]
        for k, w in enumerate(weights):
            node[k] = w
        for c in range(3):
            node[4 + c] = load(c)

        def flow(_, carry):
            for c in range(3):
                x = ext[at + c]
                total = node[4 + c]
                for k, move in enumerate((below, above, right, left)):
                    total = total + node[k] * (move(x) - x)
                ext[at + c] = jnp.where(keep, x + DT_STEP * total, 0.0)
            return carry

        lax.fori_loop(0, SUB, flow, 0)

    @pl.when(grp != 0)
    def _():
        kappa = static(0)
        kappa_up, kappa_left = above(kappa), left(kappa)
        kappa_both = left(kappa_up)
        for c in range(3):
            diagonal = (
                elem_ref[c, c] * kappa
                + elem_ref[3 + c, 3 + c] * kappa_up
                + elem_ref[6 + c, 6 + c] * kappa_left
                + elem_ref[9 + c, 9 + c] * kappa_both
            )
            diagonal = jnp.where(keep, diagonal, 1.0)
            node[12 + c] = jnp.where(keep, RELAX / diagonal, 0.0)
            node[15 + c] = load(c)

        def shell(_, carry):
            for c in range(3):
                x = ext[at + c]
                low = below(x)
                node[c] = x
                node[3 + c] = low
                node[6 + c] = right(x)
                node[9 + c] = right(low)

            def force(a):
                total = elem_ref[a, 0] * node[0]
                for b in range(1, 12):
                    total = total + elem_ref[a, b] * node[b]
                return total * static(0)

            for c in range(3):
                pull = force(c) + above(force(3 + c)) + left(force(6 + c) + above(force(9 + c)))
                ext[at + c] = ext[at + c] + node[12 + c] * (node[15 + c] - pull)
            return carry

        lax.fori_loop(0, SUB, shell, 0)

    for c in range(3):
        x = ext[at + c, 0:rows, 0:cols]
        state_out[c] = x
        table[pl.ds(c, rows, stride=8), :] = x
        table[pl.ds(4 + c, rows, stride=8), :] = x
    zero = jnp.zeros((rows, cols), jnp.float32)
    table[pl.ds(3, rows, stride=8), :] = zero
    table[pl.ds(7, rows, stride=8), :] = zero
    fetch.wait()
    batch = min(4, blocks // 2)
    line = lax.broadcasted_iota(jnp.int32, (8, cols), 0)

    def pick(step, carry):
        start = pl.multiple_of(step * (8 * batch), 8 * batch)
        cells = [source_ref[pl.ds(start + 8 * q, 8), :] for q in range(batch)]
        rows_of = [cell // cols for cell in cells]
        cols_of = [cell % cols for cell in cells]
        found = [jnp.zeros((8, cols), jnp.float32) for _ in range(batch)]
        for r in range(rows):
            line_r = table[8 * r : 8 * r + 8, :]
            for q in range(batch):
                got = jnp.take_along_axis(line_r, cols_of[q], axis=1)
                found[q] = jnp.where(rows_of[q] == r, got, found[q])
        for q in range(batch):
            upper = jnp.where(line < 4, found[q], 0.0).astype(jnp.bfloat16)
            lower = jnp.where(line < 4, 0.0, found[q]).astype(jnp.bfloat16)
            pair = step * batch + q
            matrix = map_ref[pl.ds(2 * pair, 2)].reshape(2 * cols, cols)
            mapped = jnp.dot(
                jnp.concatenate([upper, lower], axis=1), matrix, preferred_element_type=jnp.float32
            )
            mapped = jnp.where((line & 3) == 3, target_ref[pl.ds(start + 8 * q, 8), :], mapped)
            for half in range(2):
                place = slot_ref[2 * pair + half] * SLOT_ROWS
                send_out[pl.ds(place, SLOT_ROWS), :] = mapped[4 * half : 4 * half + 4]
        return carry

    lax.fori_loop(0, blocks // 2 // batch, pick, 0)


def scatter_kernel(arrived_ref, field_ref, applied_out, *outs, sizes, batch):
    rows, cols, slots = sizes
    row_id = lax.broadcasted_iota(jnp.int32, (rows, cols), 0)
    col_id = lax.broadcasted_iota(jnp.int32, (cols, cols), 0)

    def add(step, total):
        start = pl.multiple_of(step * (batch * SLOT_ROWS), batch * SLOT_ROWS)
        spread, choose = [], []
        for q in range(batch // 2):
            tile = arrived_ref[pl.ds(start + 8 * q, 8), :]
            cell = tile.astype(jnp.int32)
            cell_row, cell_col = cell // cols, cell % cols
            for half in range(2):
                at = 4 * half
                here = row_id == cell_row[at + 3 : at + 4]
                spread.append(
                    jnp.concatenate(
                        [jnp.where(here, tile[at + c : at + c + 1], 0.0) for c in range(3)], axis=0
                    ).astype(jnp.bfloat16)
                )
                choose.append(
                    jnp.where(col_id == cell_col[at + 3 : at + 4], 1.0, 0.0).astype(jnp.bfloat16)
                )
        return total + lax.dot_general(
            jnp.concatenate(spread, axis=1),
            jnp.concatenate(choose, axis=1),
            (((1,), (1,)), ((), ())),
            preferred_element_type=jnp.float32,
        )

    total = lax.fori_loop(0, slots // batch, add, jnp.zeros((3 * rows, cols), jnp.float32))
    parts = [total[rows * c : rows * (c + 1)] for c in range(3)]
    for c in range(3):
        applied_out[c] = parts[c]
    if outs:
        pack_sides([field_ref[c] for c in range(3)] + parts, *outs)


def body(
    fields,
    coefficients,
    forcing,
    element_matrix,
    source_cells,
    target_cells,
    peer_map,
    mapping_blocks,
):
    rows_x, rows_y = lax.axis_size("gx"), lax.axis_size("gy")
    state, coef, force = fields[0], coefficients[0], forcing[0]
    comps, rows, cols = state.shape
    blocks = peer_map.shape[1]
    partners = rows_x * rows_y
    slots = partners * CAPACITY
    tall, wide = rows + 2 * HALO, 2 * cols
    place = jnp.stack([lax.axis_index("grp"), lax.axis_index("gx"), lax.axis_index("gy")]).astype(
        jnp.int32
    )
    targets = peer_map[0, :, 0]
    same_peer = targets[:, None] == targets[None, :]
    earlier = lax.broadcasted_iota(jnp.int32, (blocks, blocks), 1) < lax.broadcasted_iota(
        jnp.int32, (blocks, blocks), 0
    )
    slot_of = targets * CAPACITY + jnp.sum((same_peer & earlier).astype(jnp.int32), axis=1)
    source4 = jnp.repeat(source_cells[0], SLOT_ROWS, axis=0)
    target4 = jnp.repeat(target_cells[0].astype(jnp.float32), SLOT_ROWS, axis=0)
    full = jax.ShapeDtypeStruct((comps, rows, cols), jnp.float32)
    wire = jax.ShapeDtypeStruct((slots * SLOT_ROWS, cols), jnp.float32)
    kept = jax.ShapeDtypeStruct((4, tall, wide), jnp.float32)
    grp_swap = [(0, 1), (1, 0)]

    packed = pl.pallas_call(
        first_pack_kernel, out_shape=pack_shapes(7, rows, cols), name="first_pack", interpret=INTERPRET
    )(coef, force, state)
    applied, static = None, None
    for outer in range(ITERS):
        first, last = outer == 0, outer == ITERS - 1
        sides = exchange(packed)
        lead = (coef, force, state) if first else (static, state, applied)
        swept = pl.pallas_call(
            lambda *refs, first=first: sweep_kernel(
                *refs, first=first, sizes=(rows, cols, blocks), count_x=rows_x, count_y=rows_y
            ),
            out_shape=[full, wire] + ([kept] if first else []),
            in_specs=[SMEM_SPEC] * 3 + [VMEM_SPEC] * 9 + [ANY_SPEC],
            scratch_shapes=[
                pltpu.VMEM((7 if first else 6, tall, wide), jnp.float32),
                pltpu.VMEM((tall, cols), jnp.float32),
                pltpu.VMEM((tall, cols), jnp.float32),
                pltpu.VMEM((18, tall, wide), jnp.float32),
                pltpu.VMEM((rows * 8, cols), jnp.float32),
                pltpu.VMEM(mapping_blocks.shape[1:], jnp.bfloat16),
                pltpu.SemaphoreType.DMA,
            ],
            name="sweep_first" if first else "sweep",
            interpret=INTERPRET,
        )(place, slot_of, element_matrix, *lead, *sides, source4, target4, mapping_blocks[0])
        if first:
            state, send, static = swept
        else:
            state, send = swept
        crossed = lax.ppermute(send, "grp", grp_swap)
        arrived = lax.all_to_all(
            crossed.reshape(partners, CAPACITY * SLOT_ROWS, cols),
            ("gx", "gy"),
            split_axis=0,
            concat_axis=0,
            tiled=True,
        ).reshape(slots * SLOT_ROWS, cols)
        received = pl.pallas_call(
            lambda *refs: scatter_kernel(
                *refs, sizes=(rows, cols, slots), batch=min(8, slots)
            ),
            out_shape=[full] + ([] if last else pack_shapes(6, rows, cols)),
            name="scatter_last" if last else "scatter",
            interpret=INTERPRET,
        )(arrived, state)
        applied, packed = received[0], received[1:]
    return (state[None], applied[None])


def solution(mesh):
    placed = (
        P("grp", None, "gx", "gy"),
        P("grp", "gx", "gy"),
        P("grp", None, "gx", "gy"),
        P(),
        P("grp", ("gx", "gy"), None),
        P("grp", ("gx", "gy"), None),
        P("grp", ("gx", "gy"), None),
        P("grp", ("gx", "gy"), None, None),
    )
    return jax.shard_map(
        body,
        mesh=mesh,
        in_specs=placed,
        out_specs=(P("grp", None, "gx", "gy"), P("grp", None, "gx", "gy")),
        check_vma=False,
    )
```

```python
import jax
import jax.numpy as jnp
from jax import lax
from jax.experimental import pallas as pl
from jax.experimental.pallas import tpu as pltpu
from jax.sharding import PartitionSpec as P

ITERS = 4
SUB = 4
HALO = 4
DT_STEP = 1.0
RELAX = 0.6
SLOT_ROWS = 4
CAPACITY = 2

INTERPRET = False

VMEM_SPEC = pl.BlockSpec(memory_space=pltpu.VMEM)
SMEM_SPEC = pl.BlockSpec(memory_space=pltpu.SMEM)


def near(x):
    return x if INTERPRET else pltpu.with_memory_space_constraint(x, pltpu.VMEM)


def lanes_of(shape):
    return lax.broadcasted_iota(jnp.int32, shape, len(shape) - 1)


def below(x):
    return pltpu.roll(x, x.shape[0] - 1, 0)


def above(x):
    return pltpu.roll(x, 1, 0)


def right(x):
    return pltpu.roll(x, x.shape[1] - 1, 1)


def left(x):
    return pltpu.roll(x, 1, 1)


def pack_sides(parts, left_out, right_out, top_out, bottom_out):
    rows, cols = parts[0].shape
    lane = lanes_of((rows, cols))
    low = jnp.zeros((rows, cols), jnp.float32)
    high = low
    for k, x in enumerate(parts):
        here = (lane >= HALO * k) & (lane < HALO * (k + 1))
        low = jnp.where(here, pltpu.roll(x, HALO * k, 1) if k else x, low)
        high = jnp.where(here, pltpu.roll(x, HALO * (k + 1), 1), high)
        top_out[HALO * k : HALO * (k + 1), :] = x[:HALO]
        bottom_out[HALO * k : HALO * (k + 1), :] = x[rows - HALO :]
    left_out[...] = low
    right_out[...] = high


def first_pack_kernel(coef_ref, force_ref, field_ref, left_out, right_out, top_out, bottom_out):
    parts = [coef_ref[...]] + [force_ref[c] for c in range(3)] + [field_ref[c] for c in range(3)]
    pack_sides(parts, left_out, right_out, top_out, bottom_out)


def pack_shapes(count, rows, cols):
    side = pltpu.VMEM((rows, cols), jnp.float32)
    ends = pltpu.VMEM((HALO * count, cols), jnp.float32)
    return [side, side, ends, ends]


def prepare_kernel(peer_ref, source_ref, target_ref, slot_out, source_out, target_out, seen):
    blocks = source_ref.shape[0]

    def clear(i, carry):
        seen[i] = 0
        return carry

    lax.fori_loop(0, seen.shape[0], clear, 0)

    def place(i, carry):
        peer = peer_ref[i]
        rank = seen[peer]
        slot_out[i] = peer * CAPACITY + rank
        seen[peer] = rank + 1
        return carry

    lax.fori_loop(0, blocks, place, 0)
    for k in range(SLOT_ROWS):
        source_out[pl.ds(k, blocks, stride=SLOT_ROWS), :] = source_ref[...]
        target_out[pl.ds(k, blocks, stride=SLOT_ROWS), :] = target_ref[...].astype(jnp.float32)


def edge_kernel(top_ref, bottom_ref, left_ref, right_ref, up_out, down_out):
    base, rows = top_ref.shape[0], left_ref.shape[0]
    up_out[0:base, :] = top_ref[...]
    up_out[base : base + HALO, :] = left_ref[0:HALO, :]
    up_out[base + HALO : base + 2 * HALO, :] = right_ref[0:HALO, :]
    down_out[0:base, :] = bottom_ref[...]
    down_out[base : base + HALO, :] = left_ref[rows - HALO : rows, :]
    down_out[base + HALO : base + 2 * HALO, :] = right_ref[rows - HALO : rows, :]


def exchange(packed):
    low, high, top, bottom = packed
    count_x, count_y = lax.axis_size("gx"), lax.axis_size("gy")
    up_y = [(i, (i + 1) % count_y) for i in range(count_y)]
    down_y = [(j, i) for i, j in up_y]
    up_x = [(i, (i + 1) % count_x) for i in range(count_x)]
    down_x = [(j, i) for i, j in up_x]
    from_left = lax.ppermute(high, "gy", up_y)
    from_right = lax.ppermute(low, "gy", down_y)
    ends = pltpu.VMEM((top.shape[0] + 2 * HALO, top.shape[1]), jnp.float32)
    to_up, to_down = pl.pallas_call(
        edge_kernel, out_shape=[ends, ends], name="edges", interpret=INTERPRET
    )(near(top), near(bottom), near(from_left), near(from_right))
    from_up = lax.ppermute(to_down, "gx", up_x)
    from_down = lax.ppermute(to_up, "gx", down_x)
    return from_left, from_right, from_up, from_down


def sweep_kernel(*refs, first, sizes, count_x, count_y):
    rows, cols, blocks = sizes
    tall, wide = rows + 2 * HALO, 2 * cols
    place_ref, slot_ref, elem_ref = refs[:3]
    if first:
        coef_ref, force_ref, field_ref = refs[3:6]
    else:
        static_ref, field_ref, applied_ref = refs[3:6]
    left_ref, right_ref, up_ref, down_ref, source_ref, map_ref = refs[6:12]
    if first:
        target_ref = refs[12]
    outs = refs[13:] if first else refs[12:]
    slot_rows = SLOT_ROWS if first else SLOT_ROWS - 1
    if first:
        state_out, send_out, static_out = outs[:3]
        scratch = outs[3:]
    else:
        state_out, send_out = outs[:2]
        scratch = outs[2:]
    ext, side_left, side_right, node, table = scratch
    send_out[...] = jnp.zeros(send_out.shape, jnp.float32)

    grp, place_x, place_y = place_ref[0], place_ref[1], place_ref[2]
    row_id = lax.broadcasted_iota(jnp.int32, (tall, wide), 0)
    col_id = lax.broadcasted_iota(jnp.int32, (tall, wide), 1)
    row_at = jnp.where(row_id < rows + HALO, row_id, row_id - tall) + place_x * rows
    col_in = jnp.where(col_id < cols + HALO, col_id, col_id - wide)
    col_at = col_in + place_y * cols
    keep = (row_at >= 0) & (row_at < rows * count_x) & (col_at >= 0) & (col_at < cols * count_y)
    keep = keep & (col_in >= -HALO)

    own = (
        [coef_ref[...]] + [force_ref[c] for c in range(3)] + [field_ref[c] for c in range(3)]
        if first
        else [field_ref[c] for c in range(3)] + [applied_ref[c] for c in range(3)]
    )
    count = len(own)
    base = HALO * count
    side_left[0:rows, :] = left_ref[...]
    side_left[rows : rows + HALO, :] = down_ref[base : base + HALO, :]
    side_left[rows + HALO : tall, :] = up_ref[base : base + HALO, :]
    side_right[0:rows, :] = right_ref[...]
    side_right[rows : rows + HALO, :] = down_ref[base + HALO : base + 2 * HALO, :]
    side_right[rows + HALO : tall, :] = up_ref[base + HALO : base + 2 * HALO, :]
    lane = lanes_of((tall, cols))
    for k in range(count):
        ext[k, 0:rows, 0:cols] = own[k]
        ext[k, rows : rows + HALO, 0:cols] = down_ref[HALO * k : HALO * (k + 1), :]
        ext[k, rows + HALO : tall, 0:cols] = up_ref[HALO * k : HALO * (k + 1), :]
        close = side_right[...]
        close = pltpu.roll(close, cols - HALO * k, 1) if k else close
        far = pltpu.roll(side_left[...], cols - HALO * (k + 1), 1)
        ext[k, :, cols:wide] = jnp.where(lane < HALO, close, far)
        ext[k] = jnp.where(keep, ext[k], 0.0)
    if first:
        for k in range(4):
            static_out[k] = ext[k]
        at = 4
    else:
        at = 0

    def static(k):
        return ext[k] if first else static_ref[k]

    def load(c):
        return static(1 + c) if first else static(1 + c) + ext[3 + c]

    @pl.when(grp == 0)
    def _():
        nu = static(0)
        weights = [0.5 * (nu + move(nu)) for move in (below, above, right, left)]
        for k, w in enumerate(weights):
            node[k] = w
        for c in range(3):
            node[4 + c] = load(c)

        def flow(_, carry):
            for c in range(3):
                x = ext[at + c]
                total = node[4 + c]
                for k, move in enumerate((below, above, right, left)):
                    total = total + node[k] * (move(x) - x)
                ext[at + c] = jnp.where(keep, x + DT_STEP * total, 0.0)
            return carry

        lax.fori_loop(0, SUB, flow, 0)

    @pl.when(grp != 0)
    def _():
        kappa = static(0)
        kappa_up, kappa_left = above(kappa), left(kappa)
        kappa_both = left(kappa_up)
        for c in range(3):
            diagonal = (
                elem_ref[c, c] * kappa
                + elem_ref[3 + c, 3 + c] * kappa_up
                + elem_ref[6 + c, 6 + c] * kappa_left
                + elem_ref[9 + c, 9 + c] * kappa_both
            )
            diagonal = jnp.where(keep, diagonal, 1.0)
            node[12 + c] = jnp.where(keep, RELAX / diagonal, 0.0)
            node[15 + c] = load(c)

        def shell(_, carry):
            for c in range(3):
                x = ext[at + c]
                low = below(x)
                node[c] = x
                node[3 + c] = low
                node[6 + c] = right(x)
                node[9 + c] = right(low)

            def force(a):
                total = elem_ref[a, 0] * node[0]
                for b in range(1, 12):
                    total = total + elem_ref[a, b] * node[b]
                return total * static(0)

            for c in range(3):
                pull = force(c) + above(force(3 + c)) + left(force(6 + c) + above(force(9 + c)))
                ext[at + c] = ext[at + c] + node[12 + c] * (node[15 + c] - pull)
            return carry

        lax.fori_loop(0, SUB, shell, 0)

    for c in range(3):
        x = ext[at + c, 0:rows, 0:cols]
        state_out[c] = x
        table[pl.ds(c, rows, stride=8), :] = x
        table[pl.ds(4 + c, rows, stride=8), :] = x
    zero = jnp.zeros((rows, cols), jnp.float32)
    table[pl.ds(3, rows, stride=8), :] = zero
    table[pl.ds(7, rows, stride=8), :] = zero
    batch = min(4, blocks // 2)
    line = lax.broadcasted_iota(jnp.int32, (8, cols), 0)

    def pick(step, carry):
        start = pl.multiple_of(step * (8 * batch), 8 * batch)
        cells = [source_ref[pl.ds(start + 8 * q, 8), :] for q in range(batch)]
        rows_of = [cell // cols for cell in cells]
        cols_of = [cell % cols for cell in cells]
        found = [jnp.zeros((8, cols), jnp.float32) for _ in range(batch)]
        for r in range(rows):
            line_r = table[8 * r : 8 * r + 8, :]
            for q in range(batch):
                got = jnp.take_along_axis(line_r, cols_of[q], axis=1)
                found[q] = jnp.where(rows_of[q] == r, got, found[q])
        for q in range(batch):
            upper = jnp.where(line < 4, found[q], 0.0).astype(jnp.bfloat16)
            lower = jnp.where(line < 4, 0.0, found[q]).astype(jnp.bfloat16)
            pair = step * batch + q
            matrix = map_ref[pl.ds(2 * pair, 2)].reshape(2 * cols, cols)
            mapped = jnp.dot(
                jnp.concatenate([upper, lower], axis=1), matrix, preferred_element_type=jnp.float32
            )
            if first:
                cell = target_ref[pl.ds(start + 8 * q, 8), :]
                mapped = jnp.where((line & 3) == 3, cell, mapped)
            for half in range(2):
                place = slot_ref[2 * pair + half] * slot_rows
                send_out[pl.ds(place, slot_rows), :] = mapped[4 * half : 4 * half + slot_rows]
        return carry

    lax.fori_loop(0, blocks // 2 // batch, pick, 0)


def scatter_kernel(arrived_ref, *refs, first, last, sizes, batch):
    rows, cols, slots = sizes
    refs = list(refs)
    cells_ref = None if first else refs.pop(0)
    field_ref = None if last else refs.pop(0)
    applied_out = refs.pop(0)
    slot_rows = SLOT_ROWS if first else SLOT_ROWS - 1
    if first:
        cells_out = refs.pop(0)
        cells_out[...] = arrived_ref[pl.ds(SLOT_ROWS - 1, slots, stride=SLOT_ROWS), :].astype(jnp.int32)
        cells_ref = cells_out
    row_id = lax.broadcasted_iota(jnp.int32, (rows, cols), 0)
    col_id = lax.broadcasted_iota(jnp.int32, (cols, cols), 0)
    group = 8

    def add(step, total):
        spread, choose = [], []
        for part in range(batch // group):
            slot = pl.multiple_of(step * batch + part * group, group)
            cell = cells_ref[pl.ds(slot, group), :]
            cell_row, cell_col = cell // cols, cell % cols
            tile = arrived_ref[pl.ds(pl.multiple_of(slot * slot_rows, 8), group * slot_rows), :]
            for q in range(group):
                at = q * slot_rows
                here = row_id == cell_row[q : q + 1]
                spread.append(
                    jnp.concatenate(
                        [jnp.where(here, tile[at + c : at + c + 1], 0.0) for c in range(3)], axis=0
                    ).astype(jnp.bfloat16)
                )
                choose.append(
                    jnp.where(col_id == cell_col[q : q + 1], 1.0, 0.0).astype(jnp.bfloat16)
                )
        return total + lax.dot_general(
            jnp.concatenate(spread, axis=1),
            jnp.concatenate(choose, axis=1),
            (((1,), (1,)), ((), ())),
            preferred_element_type=jnp.float32,
        )

    total = lax.fori_loop(0, slots // batch, add, jnp.zeros((3 * rows, cols), jnp.float32))
    parts = [total[rows * c : rows * (c + 1)] for c in range(3)]
    for c in range(3):
        applied_out[c] = parts[c]
    if not last:
        pack_sides([field_ref[c] for c in range(3)] + parts, *refs)


def body(
    fields,
    coefficients,
    forcing,
    element_matrix,
    source_cells,
    target_cells,
    peer_map,
    mapping_blocks,
):
    rows_x, rows_y = lax.axis_size("gx"), lax.axis_size("gy")
    state, coef, force = fields[0], coefficients[0], forcing[0]
    comps, rows, cols = state.shape
    blocks = peer_map.shape[1]
    partners = rows_x * rows_y
    slots = partners * CAPACITY
    tall, wide = rows + 2 * HALO, 2 * cols
    place = jnp.stack([lax.axis_index("grp"), lax.axis_index("gx"), lax.axis_index("gy")]).astype(
        jnp.int32
    )
    full = pltpu.VMEM((comps, rows, cols), jnp.float32)
    full_hbm = jax.ShapeDtypeStruct((comps, rows, cols), jnp.float32)
    kept = pltpu.VMEM((4, tall, wide), jnp.float32)
    grp_swap = [(0, 1), (1, 0)]

    packed = pl.pallas_call(
        first_pack_kernel, out_shape=pack_shapes(7, rows, cols), name="first_pack", interpret=INTERPRET
    )(coef, force, state)
    slot_of, source4, target4 = pl.pallas_call(
        prepare_kernel,
        out_shape=[
            jax.ShapeDtypeStruct((blocks,), jnp.int32),
            pltpu.VMEM((blocks * SLOT_ROWS, cols), jnp.int32),
            pltpu.VMEM((blocks * SLOT_ROWS, cols), jnp.float32),
        ],
        in_specs=[SMEM_SPEC, VMEM_SPEC, VMEM_SPEC],
        out_specs=[SMEM_SPEC, VMEM_SPEC, VMEM_SPEC],
        scratch_shapes=[pltpu.SMEM((partners,), jnp.int32)],
        name="prepare",
        interpret=INTERPRET,
    )(peer_map[0, :, 0], source_cells[0], target_cells[0])
    applied, static, cells = None, None, None
    for outer in range(ITERS):
        first, last = outer == 0, outer == ITERS - 1
        sides = exchange(packed)
        slot_rows = SLOT_ROWS if first else SLOT_ROWS - 1
        wire = pltpu.VMEM((slots * slot_rows, cols), jnp.float32)
        lead = (coef, force, state) if first else (static, state, applied)
        swept = pl.pallas_call(
            lambda *refs, first=first: sweep_kernel(
                *refs, first=first, sizes=(rows, cols, blocks), count_x=rows_x, count_y=rows_y
            ),
            out_shape=[full_hbm if last else full, wire] + ([kept] if first else []),
            in_specs=[SMEM_SPEC] * 3 + [VMEM_SPEC] * (10 if first else 9),
            scratch_shapes=[
                pltpu.VMEM((7 if first else 6, tall, wide), jnp.float32),
                pltpu.VMEM((tall, cols), jnp.float32),
                pltpu.VMEM((tall, cols), jnp.float32),
                pltpu.VMEM((18, tall, wide), jnp.float32),
                pltpu.VMEM((rows * 8, cols), jnp.float32),
            ],
            name="sweep_first" if first else "sweep",
            interpret=INTERPRET,
        )(
            place,
            slot_of,
            element_matrix,
            *(lead if first else map(near, lead)),
            *map(near, sides),
            near(source4),
            near(mapping_blocks[0]),
            *([near(target4)] if first else []),
        )
        if first:
            state, send, static = swept
        else:
            state, send = swept
        crossed = lax.ppermute(send, "grp", grp_swap)
        arrived = lax.all_to_all(
            crossed.reshape((partners, CAPACITY * SLOT_ROWS, cols) if first else (partners, 3, CAPACITY, cols)),
            ("gx", "gy"),
            split_axis=0,
            concat_axis=0,
            tiled=True,
        ).reshape(slots * slot_rows, cols)
        received = pl.pallas_call(
            lambda *refs, first=first, last=last: scatter_kernel(
                *refs, first=first, last=last, sizes=(rows, cols, slots), batch=min(64, slots)
            ),
            out_shape=[full_hbm if last else full]
            + ([pltpu.VMEM((slots, cols), jnp.int32)] if first else [])
            + ([] if last else pack_shapes(6, rows, cols)),
            name="scatter_first" if first else "scatter_last" if last else "scatter",
            interpret=INTERPRET,
        )(near(arrived), *([] if first else [near(cells)]), *([] if last else [near(state)]))
        applied, packed = received[0], received[1:]
        if first:
            cells, packed = packed[0], packed[1:]
    return (state[None], applied[None])


def solution(mesh):
    placed = (
        P("grp", None, "gx", "gy"),
        P("grp", "gx", "gy"),
        P("grp", None, "gx", "gy"),
        P(),
        P("grp", ("gx", "gy"), None),
        P("grp", ("gx", "gy"), None),
        P("grp", ("gx", "gy"), None),
        P("grp", ("gx", "gy"), None, None),
    )
    return jax.shard_map(
        body,
        mesh=mesh,
        in_specs=placed,
        out_specs=(P("grp", None, "gx", "gy"), P("grp", None, "gx", "gy")),
        check_vma=False,
    )
```

```python
import jax
import jax.numpy as jnp
from jax import lax
from jax.experimental import pallas as pl
from jax.experimental.pallas import tpu as pltpu
from jax.sharding import PartitionSpec as P

ITERS = 4
SUB = 4
HALO = 4
DT_STEP = 1.0
RELAX = 0.6
SLOT_ROWS = 4
CAPACITY = 2
PICK_BATCH = 4
MAP_BATCH = 8
SCATTER_BATCH = 128

INTERPRET = False

VMEM_SPEC = pl.BlockSpec(memory_space=pltpu.VMEM)
SMEM_SPEC = pl.BlockSpec(memory_space=pltpu.SMEM)


def near(x):
    return x if INTERPRET else pltpu.with_memory_space_constraint(x, pltpu.VMEM)


def lanes_of(shape):
    return lax.broadcasted_iota(jnp.int32, shape, len(shape) - 1)


def below(x):
    return pltpu.roll(x, x.shape[0] - 1, 0)


def above(x):
    return pltpu.roll(x, 1, 0)


def right(x):
    return pltpu.roll(x, x.shape[1] - 1, 1)


def left(x):
    return pltpu.roll(x, 1, 1)


def pack_sides(parts, left_out, right_out, top_out, bottom_out):
    rows, cols = parts[0].shape
    lane = lanes_of((rows, cols))
    low = jnp.zeros((rows, cols), jnp.float32)
    high = low
    for k, x in enumerate(parts):
        here = (lane >= HALO * k) & (lane < HALO * (k + 1))
        low = jnp.where(here, pltpu.roll(x, HALO * k, 1) if k else x, low)
        high = jnp.where(here, pltpu.roll(x, HALO * (k + 1), 1), high)
        top_out[HALO * k : HALO * (k + 1), :] = x[:HALO]
        bottom_out[HALO * k : HALO * (k + 1), :] = x[rows - HALO :]
    left_out[...] = low
    right_out[...] = high


def first_pack_kernel(coef_ref, force_ref, field_ref, left_out, right_out, top_out, bottom_out):
    parts = [coef_ref[...]] + [force_ref[c] for c in range(3)] + [field_ref[c] for c in range(3)]
    pack_sides(parts, left_out, right_out, top_out, bottom_out)


def pack_shapes(count, rows, cols):
    side = pltpu.VMEM((rows, cols), jnp.float32)
    ends = pltpu.VMEM((HALO * count, cols), jnp.float32)
    return [side, side, ends, ends]


def prepare_kernel(
    peer_ref, source_hbm, target_hbm, map_hbm, slot_out, source_out, target_out, map_out, seen, sems
):
    fetches = [
        pltpu.make_async_copy(source, target, sems.at[k])
        for k, (source, target) in enumerate(
            ((source_hbm, source_out), (target_hbm, target_out), (map_hbm, map_out))
        )
    ]
    for fetch in fetches:
        fetch.start()

    def clear(i, carry):
        seen[i] = 0
        return carry

    lax.fori_loop(0, seen.shape[0], clear, 0, unroll=16)

    def place(i, carry):
        peer = peer_ref[i]
        rank = seen[peer]
        slot_out[i] = peer * CAPACITY + rank
        seen[peer] = rank + 1
        return carry

    lax.fori_loop(0, peer_ref.shape[0], place, 0, unroll=8)
    for fetch in fetches:
        fetch.wait()


def edge_kernel(top_ref, bottom_ref, left_ref, right_ref, *refs):
    up_out, down_out = refs[-2:]
    base, rows = top_ref.shape[0], left_ref.shape[0]
    up_out[0:base, :] = top_ref[...]
    up_out[base : base + HALO, :] = left_ref[0:HALO, :]
    up_out[base + HALO : base + 2 * HALO, :] = right_ref[0:HALO, :]
    down_out[0:base, :] = bottom_ref[...]
    down_out[base : base + HALO, :] = left_ref[rows - HALO : rows, :]
    down_out[base + HALO : base + 2 * HALO, :] = right_ref[rows - HALO : rows, :]


def exchange(packed, *after):
    low, high, top, bottom = packed
    count_x, count_y = lax.axis_size("gx"), lax.axis_size("gy")
    up_y = [(i, (i + 1) % count_y) for i in range(count_y)]
    down_y = [(j, i) for i, j in up_y]
    up_x = [(i, (i + 1) % count_x) for i in range(count_x)]
    down_x = [(j, i) for i, j in up_x]
    from_left = lax.ppermute(high, "gy", up_y)
    from_right = lax.ppermute(low, "gy", down_y)
    ends = pltpu.VMEM((top.shape[0] + 2 * HALO, top.shape[1]), jnp.float32)
    to_up, to_down = pl.pallas_call(
        edge_kernel,
        out_shape=[ends, ends],
        in_specs=[VMEM_SPEC] * 4 + [SMEM_SPEC] * len(after),
        name="edges_first" if after else "edges",
        interpret=INTERPRET,
    )(near(top), near(bottom), near(from_left), near(from_right), *after)
    from_up = lax.ppermute(to_down, "gx", up_x)
    from_down = lax.ppermute(to_up, "gx", down_x)
    return from_left, from_right, from_up, from_down


def sweep_kernel(*refs, first, sizes, count_x, count_y):
    rows, cols, blocks = sizes
    tall, wide = rows + 2 * HALO, 2 * cols
    place_ref, slot_ref, elem_ref = refs[:3]
    if first:
        coef_ref, force_ref, field_ref = refs[3:6]
    else:
        static_ref, field_ref, applied_ref = refs[3:6]
    left_ref, right_ref, up_ref, down_ref, source_ref, map_ref = refs[6:12]
    if first:
        target_ref = refs[12]
    outs = refs[13:] if first else refs[12:]
    slot_rows = SLOT_ROWS if first else SLOT_ROWS - 1
    if first:
        state_out, send_out, static_out = outs[:3]
        scratch = outs[3:]
    else:
        state_out, send_out = outs[:2]
        scratch = outs[2:]
    ext, side_left, side_right, node, reads = scratch
    send_out[...] = jnp.zeros(send_out.shape, jnp.float32)

    grp, place_x, place_y = place_ref[0], place_ref[1], place_ref[2]
    row_id = lax.broadcasted_iota(jnp.int32, (tall, wide), 0)
    col_id = lax.broadcasted_iota(jnp.int32, (tall, wide), 1)
    row_at = jnp.where(row_id < rows + HALO, row_id, row_id - tall) + place_x * rows
    col_in = jnp.where(col_id < cols + HALO, col_id, col_id - wide)
    col_at = col_in + place_y * cols
    keep = (row_at >= 0) & (row_at < rows * count_x) & (col_at >= 0) & (col_at < cols * count_y)
    keep = keep & (col_in >= -HALO)

    own = (
        [coef_ref[...]] + [force_ref[c] for c in range(3)] + [field_ref[c] for c in range(3)]
        if first
        else [field_ref[c] for c in range(3)] + [applied_ref[c] for c in range(3)]
    )
    count = len(own)
    base = HALO * count
    side_left[0:rows, :] = left_ref[...]
    side_left[rows : rows + HALO, :] = down_ref[base : base + HALO, :]
    side_left[rows + HALO : tall, :] = up_ref[base : base + HALO, :]
    side_right[0:rows, :] = right_ref[...]
    side_right[rows : rows + HALO, :] = down_ref[base + HALO : base + 2 * HALO, :]
    side_right[rows + HALO : tall, :] = up_ref[base + HALO : base + 2 * HALO, :]
    lane = lanes_of((tall, cols))
    for k in range(count):
        ext[k, 0:rows, 0:cols] = own[k]
        ext[k, rows : rows + HALO, 0:cols] = down_ref[HALO * k : HALO * (k + 1), :]
        ext[k, rows + HALO : tall, 0:cols] = up_ref[HALO * k : HALO * (k + 1), :]
        close = side_right[...]
        close = pltpu.roll(close, cols - HALO * k, 1) if k else close
        far = pltpu.roll(side_left[...], cols - HALO * (k + 1), 1)
        ext[k, :, cols:wide] = jnp.where(lane < HALO, close, far)
        ext[k] = jnp.where(keep, ext[k], 0.0)
    if first:
        for k in range(4):
            static_out[k] = ext[k]
        at = 4
    else:
        at = 0

    def static(k):
        return ext[k] if first else static_ref[k]

    def load(c):
        return static(1 + c) if first else static(1 + c) + ext[3 + c]

    @pl.when(grp == 0)
    def _():
        nu = static(0)
        weights = [0.5 * (nu + move(nu)) for move in (below, above, right, left)]
        for k, w in enumerate(weights):
            node[k] = w
        for c in range(3):
            node[4 + c] = load(c)

        def flow(_, carry):
            for c in range(3):
                x = ext[at + c]
                total = node[4 + c]
                for k, move in enumerate((below, above, right, left)):
                    total = total + node[k] * (move(x) - x)
                ext[at + c] = jnp.where(keep, x + DT_STEP * total, 0.0)
            return carry

        lax.fori_loop(0, SUB, flow, 0)

    @pl.when(grp != 0)
    def _():
        kappa = static(0)
        kappa_up, kappa_left = above(kappa), left(kappa)
        kappa_both = left(kappa_up)
        for c in range(3):
            diagonal = (
                elem_ref[c, c] * kappa
                + elem_ref[3 + c, 3 + c] * kappa_up
                + elem_ref[6 + c, 6 + c] * kappa_left
                + elem_ref[9 + c, 9 + c] * kappa_both
            )
            diagonal = jnp.where(keep, diagonal, 1.0)
            node[12 + c] = jnp.where(keep, RELAX / diagonal, 0.0)
            node[15 + c] = load(c)

        def shell(_, carry):
            for c in range(3):
                x = ext[at + c]
                low = below(x)
                node[c] = x
                node[3 + c] = low
                node[6 + c] = right(x)
                node[9 + c] = right(low)

            def force(a):
                total = elem_ref[a, 0] * node[0]
                for b in range(1, 12):
                    total = total + elem_ref[a, b] * node[b]
                return total * static(0)

            for c in range(3):
                pull = force(c) + above(force(3 + c)) + left(force(6 + c) + above(force(9 + c)))
                ext[at + c] = ext[at + c] + node[12 + c] * (node[15 + c] - pull)
            return carry

        lax.fori_loop(0, SUB, shell, 0)

    for c in range(3):
        state_out[c] = ext[at + c, 0:rows, 0:cols]
    group = 8
    batch = min(PICK_BATCH, blocks // group)

    def pick(step, carry):
        for q in range(batch):
            start = pl.multiple_of((step * batch + q) * group, group)
            cell = source_ref[pl.ds(start, group), :]
            row_of, col_of = cell // cols, cell % cols
            found = [jnp.zeros((group, cols), jnp.float32) for _ in range(3)]
            for r in range(rows):
                here = row_of == r
                for c in range(3):
                    line = jnp.broadcast_to(ext[at + c, r : r + 1, 0:cols], (group, cols))
                    got = jnp.take_along_axis(line, col_of, axis=1)
                    found[c] = jnp.where(here, got, found[c])
            for c in range(3):
                reads[pl.ds(3 * start + c * group, group), :] = found[c]
        return carry

    lax.fori_loop(0, blocks // group // batch, pick, 0)
    chunk = min(MAP_BATCH, blocks // group)
    block_id = lax.broadcasted_iota(jnp.int32, (3 * group, cols), 0) % group

    def send(step, carry):
        for q in range(chunk):
            start = pl.multiple_of((step * chunk + q) * group, group)
            read = reads[pl.ds(3 * start, 3 * group), :]
            for k in range(0, group, 2):
                halves = [jnp.where(block_id == k + h, read, 0.0).astype(jnp.bfloat16) for h in range(2)]
                matrix = map_ref[pl.ds(start + k, 2)].reshape(2 * cols, cols)
                mapped = jnp.dot(
                    jnp.concatenate(halves, axis=1), matrix, preferred_element_type=jnp.float32
                )
                for h in range(2):
                    place = slot_ref[start + k + h] * slot_rows
                    for c in range(3):
                        at_row = c * group + k + h
                        send_out[pl.ds(place + c, 1), :] = mapped[at_row : at_row + 1]
                    if first:
                        send_out[pl.ds(place + 3, 1), :] = target_ref[
                            pl.ds(start + k + h, 1), :
                        ].astype(jnp.float32)
        return carry

    lax.fori_loop(0, blocks // group // chunk, send, 0)


def scatter_kernel(arrived_ref, *refs, first, last, sizes, batch):
    rows, cols, slots = sizes
    refs = list(refs)
    cells_ref = None if first else refs.pop(0)
    field_ref = None if last else refs.pop(0)
    applied_out = refs.pop(0)
    slot_rows = SLOT_ROWS if first else SLOT_ROWS - 1
    if first:
        cells_out = refs.pop(0)
        cells_out[...] = arrived_ref[pl.ds(SLOT_ROWS - 1, slots, stride=SLOT_ROWS), :].astype(jnp.int32)
        cells_ref = cells_out
    row_id = lax.broadcasted_iota(jnp.int32, (rows, cols), 0)
    col_id = lax.broadcasted_iota(jnp.int32, (cols, cols), 0)
    group = 8

    def add(step, total):
        spread, choose = [], []
        for part in range(batch // group):
            slot = pl.multiple_of(step * batch + part * group, group)
            cell = cells_ref[pl.ds(slot, group), :]
            cell_row, cell_col = cell // cols, cell % cols
            tile = arrived_ref[pl.ds(pl.multiple_of(slot * slot_rows, 8), group * slot_rows), :]
            for q in range(group):
                at = q * slot_rows
                here = row_id == cell_row[q : q + 1]
                spread.append(
                    jnp.concatenate(
                        [jnp.where(here, tile[at + c : at + c + 1], 0.0) for c in range(3)], axis=0
                    ).astype(jnp.bfloat16)
                )
                choose.append(
                    jnp.where(col_id == cell_col[q : q + 1], 1.0, 0.0).astype(jnp.bfloat16)
                )
        return total + lax.dot_general(
            jnp.concatenate(spread, axis=1),
            jnp.concatenate(choose, axis=1),
            (((1,), (1,)), ((), ())),
            preferred_element_type=jnp.float32,
        )

    total = lax.fori_loop(0, slots // batch, add, jnp.zeros((3 * rows, cols), jnp.float32))
    parts = [total[rows * c : rows * (c + 1)] for c in range(3)]
    for c in range(3):
        applied_out[c] = parts[c]
    if not last:
        pack_sides([field_ref[c] for c in range(3)] + parts, *refs)


def body(
    fields,
    coefficients,
    forcing,
    element_matrix,
    source_cells,
    target_cells,
    peer_map,
    mapping_blocks,
):
    rows_x, rows_y = lax.axis_size("gx"), lax.axis_size("gy")
    state, coef, force = fields[0], coefficients[0], forcing[0]
    comps, rows, cols = state.shape
    blocks = peer_map.shape[1]
    partners = rows_x * rows_y
    slots = partners * CAPACITY
    tall, wide = rows + 2 * HALO, 2 * cols
    place = jnp.stack([lax.axis_index("grp"), lax.axis_index("gx"), lax.axis_index("gy")]).astype(
        jnp.int32
    )
    full = pltpu.VMEM((comps, rows, cols), jnp.float32)
    full_hbm = jax.ShapeDtypeStruct((comps, rows, cols), jnp.float32)
    kept = pltpu.VMEM((4, tall, wide), jnp.float32)
    grp_swap = [(0, 1), (1, 0)]

    packed = pl.pallas_call(
        first_pack_kernel, out_shape=pack_shapes(7, rows, cols), name="first_pack", interpret=INTERPRET
    )(coef, force, state)
    slot_of, source, target, matrices = pl.pallas_call(
        prepare_kernel,
        out_shape=[
            jax.ShapeDtypeStruct((blocks,), jnp.int32),
            pltpu.VMEM((blocks, cols), jnp.int32),
            pltpu.VMEM((blocks, cols), jnp.int32),
            pltpu.VMEM(mapping_blocks.shape[1:], jnp.bfloat16),
        ],
        in_specs=[SMEM_SPEC] + [pl.BlockSpec(memory_space=pl.ANY)] * 3,
        out_specs=[SMEM_SPEC, VMEM_SPEC, VMEM_SPEC, VMEM_SPEC],
        scratch_shapes=[pltpu.SMEM((partners,), jnp.int32), pltpu.SemaphoreType.DMA((3,))],
        name="prepare",
        interpret=INTERPRET,
    )(peer_map[0, :, 0], source_cells[0], target_cells[0], mapping_blocks[0])
    applied, static, cells = None, None, None
    for outer in range(ITERS):
        first, last = outer == 0, outer == ITERS - 1
        sides = exchange(packed, *([slot_of, place] if first else []))
        slot_rows = SLOT_ROWS if first else SLOT_ROWS - 1
        wire = pltpu.VMEM((slots * slot_rows, cols), jnp.float32)
        lead = (coef, force, state) if first else (static, state, applied)
        swept = pl.pallas_call(
            lambda *refs, first=first: sweep_kernel(
                *refs, first=first, sizes=(rows, cols, blocks), count_x=rows_x, count_y=rows_y
            ),
            out_shape=[full_hbm if last else full, wire] + ([kept] if first else []),
            in_specs=[SMEM_SPEC] * 3 + [VMEM_SPEC] * (10 if first else 9),
            scratch_shapes=[
                pltpu.VMEM((7 if first else 6, tall, wide), jnp.float32),
                pltpu.VMEM((tall, cols), jnp.float32),
                pltpu.VMEM((tall, cols), jnp.float32),
                pltpu.VMEM((18, tall, wide), jnp.float32),
                pltpu.VMEM((blocks * 3, cols), jnp.float32),
            ],
            name="sweep_first" if first else "sweep",
            interpret=INTERPRET,
        )(
            place,
            slot_of,
            element_matrix,
            *(lead if first else map(near, lead)),
            *map(near, sides),
            near(source),
            near(matrices),
            *([near(target)] if first else []),
        )
        if first:
            state, send, static = swept
        else:
            state, send = swept
        crossed = lax.ppermute(send, "grp", grp_swap)
        arrived = lax.all_to_all(
            crossed.reshape((partners, CAPACITY * SLOT_ROWS, cols) if first else (partners, 3, CAPACITY, cols)),
            ("gx", "gy"),
            split_axis=0,
            concat_axis=0,
            tiled=True,
        ).reshape(slots * slot_rows, cols)
        received = pl.pallas_call(
            lambda *refs, first=first, last=last: scatter_kernel(
                *refs, first=first, last=last, sizes=(rows, cols, slots), batch=min(SCATTER_BATCH, slots)
            ),
            out_shape=[full_hbm if last else full]
            + ([pltpu.VMEM((slots, cols), jnp.int32)] if first else [])
            + ([] if last else pack_shapes(6, rows, cols)),
            name="scatter_first" if first else "scatter_last" if last else "scatter",
            interpret=INTERPRET,
        )(near(arrived), *([] if first else [near(cells)]), *([] if last else [near(state)]))
        applied, packed = received[0], received[1:]
        if first:
            cells, packed = packed[0], packed[1:]
    return (state[None], applied[None])


def solution(mesh):
    placed = (
        P("grp", None, "gx", "gy"),
        P("grp", "gx", "gy"),
        P("grp", None, "gx", "gy"),
        P(),
        P("grp", ("gx", "gy"), None),
        P("grp", ("gx", "gy"), None),
        P("grp", ("gx", "gy"), None),
        P("grp", ("gx", "gy"), None, None),
    )
    return jax.shard_map(
        body,
        mesh=mesh,
        in_specs=placed,
        out_specs=(P("grp", None, "gx", "gy"), P("grp", None, "gx", "gy")),
        check_vma=False,
    )
```

```python
import jax
import jax.numpy as jnp
from jax import lax
from jax.experimental import pallas as pl
from jax.experimental.pallas import tpu as pltpu
from jax.sharding import PartitionSpec as P

ITERS = 4
SUB = 4
HALO = 4
DT_STEP = 1.0
RELAX = 0.6
SLOT_ROWS = 4
CAPACITY = 2
PICK_BATCH = 4
MAP_BATCH = 8
SCATTER_BATCH = 128

INTERPRET = False

VMEM_SPEC = pl.BlockSpec(memory_space=pltpu.VMEM)
ANY_SPEC = pl.BlockSpec(memory_space=pl.ANY)
SMEM_SPEC = pl.BlockSpec(memory_space=pltpu.SMEM)


def near(x):
    return x if INTERPRET else pltpu.with_memory_space_constraint(x, pltpu.VMEM)


def lanes_of(shape):
    return lax.broadcasted_iota(jnp.int32, shape, len(shape) - 1)


def below(x):
    return pltpu.roll(x, x.shape[0] - 1, 0)


def above(x):
    return pltpu.roll(x, 1, 0)


def right(x):
    return pltpu.roll(x, x.shape[1] - 1, 1)


def left(x):
    return pltpu.roll(x, 1, 1)


def pack_sides(parts, place_ref, even_out, odd_out, top_out, bottom_out):
    rows, cols = parts[0].shape
    lane = lanes_of((rows, cols))
    low = jnp.zeros((rows, cols), jnp.float32)
    high = low
    for k, x in enumerate(parts):
        here = (lane >= HALO * k) & (lane < HALO * (k + 1))
        low = jnp.where(here, pltpu.roll(x, HALO * k, 1) if k else x, low)
        high = jnp.where(here, pltpu.roll(x, HALO * (k + 1), 1), high)
        top_out[HALO * k : HALO * (k + 1), :] = x[:HALO]
        bottom_out[HALO * k : HALO * (k + 1), :] = x[rows - HALO :]
    is_even = place_ref[2] % 2 == 0
    even_out[...] = jnp.where(is_even, high, low)
    odd_out[...] = jnp.where(is_even, low, high)


def first_pack_kernel(place_ref, coef_ref, force_ref, field_ref, *outs):
    parts = [coef_ref[...]] + [force_ref[c] for c in range(3)] + [field_ref[c] for c in range(3)]
    pack_sides(parts, place_ref, *outs)


def pack_shapes(count, rows, cols):
    side = pltpu.VMEM((rows, cols), jnp.float32)
    ends = pltpu.VMEM((HALO * count, cols), jnp.float32)
    return [side, side, ends, ends]


def prepare_kernel(
    peer_ref, source_hbm, target_hbm, slot_out, source_out, target_out, seen, sems
):
    fetches = [
        pltpu.make_async_copy(source, target, sems.at[k])
        for k, (source, target) in enumerate(
            ((source_hbm, source_out), (target_hbm, target_out))
        )
    ]
    for fetch in fetches:
        fetch.start()

    def clear(i, carry):
        seen[i] = 0
        return carry

    lax.fori_loop(0, seen.shape[0], clear, 0, unroll=16)

    def place(i, carry):
        peer = peer_ref[i]
        rank = seen[peer]
        slot_out[i] = peer * CAPACITY + rank
        seen[peer] = rank + 1
        return carry

    lax.fori_loop(0, peer_ref.shape[0], place, 0, unroll=8)
    for fetch in fetches:
        fetch.wait()


def edge_kernel(place_ref, top_ref, bottom_ref, even_ref, odd_ref, *refs):
    even_out, odd_out = refs[-2:]
    base, rows = top_ref.shape[0], even_ref.shape[0]
    row_even, col_even = place_ref[1] % 2 == 0, place_ref[2] % 2 == 0
    even_in, odd_in = even_ref[...], odd_ref[...]
    from_left = jnp.where(col_even, odd_in, even_in)
    from_right = jnp.where(col_even, even_in, odd_in)

    def put(start, stop, upper, lower):
        even_out[start:stop, :] = jnp.where(row_even, lower, upper)
        odd_out[start:stop, :] = jnp.where(row_even, upper, lower)

    put(0, base, top_ref[...], bottom_ref[...])
    put(base, base + HALO, from_left[:HALO], from_left[rows - HALO :])
    put(base + HALO, base + 2 * HALO, from_right[:HALO], from_right[rows - HALO :])


def swap_even(value, axis):
    return lax.ppermute(value, axis, [(i, i ^ 1) for i in range(lax.axis_size(axis))])


def swap_odd(value, axis):
    count = lax.axis_size(axis)
    return lax.ppermute(value, axis, [(i, (((i + 1) ^ 1) - 1) % count) for i in range(count)])


def exchange(packed, place, *after):
    even, odd, top, bottom = packed
    even, odd = swap_even(even, "gy"), swap_odd(odd, "gy")
    ends = pltpu.VMEM((top.shape[0] + 2 * HALO, top.shape[1]), jnp.float32)
    row_even, row_odd = pl.pallas_call(
        edge_kernel,
        out_shape=[ends, ends],
        in_specs=[SMEM_SPEC] + [VMEM_SPEC] * 4 + [SMEM_SPEC] * len(after),
        name="edges_first" if after else "edges",
        interpret=INTERPRET,
    )(place, near(top), near(bottom), near(even), near(odd), *after)
    row_odd = swap_odd(row_odd, "gx")
    row_even = swap_even(row_even, "gx")
    return even, odd, row_even, row_odd


def sweep_kernel(*refs, first, sizes, count_x, count_y):
    rows, cols, blocks = sizes
    tall, wide = rows + 2 * HALO, 2 * cols
    place_ref, slot_ref, elem_ref = refs[:3]
    if first:
        coef_ref, force_ref, field_ref = refs[3:6]
    else:
        static_ref, field_ref, applied_ref = refs[3:6]
    even_ref, odd_ref, row_even_ref, row_odd_ref, source_ref, map_hbm = refs[6:12]
    if first:
        target_ref = refs[12]
    outs = refs[13:] if first else refs[12:]
    slot_rows = SLOT_ROWS if first else SLOT_ROWS - 1
    if first:
        state_out, send_out, static_out = outs[:3]
        scratch = outs[3:]
    else:
        state_out, send_out = outs[:2]
        scratch = outs[2:]
    ext, side_left, side_right, node, reads, map_ref, map_sem = scratch
    fetch = pltpu.make_async_copy(map_hbm, map_ref, map_sem)
    fetch.start()
    send_out[...] = jnp.zeros(send_out.shape, jnp.float32)

    grp, place_x, place_y = place_ref[0], place_ref[1], place_ref[2]
    row_id = lax.broadcasted_iota(jnp.int32, (tall, wide), 0)
    col_id = lax.broadcasted_iota(jnp.int32, (tall, wide), 1)
    row_at = jnp.where(row_id < rows + HALO, row_id, row_id - tall) + place_x * rows
    col_in = jnp.where(col_id < cols + HALO, col_id, col_id - wide)
    col_at = col_in + place_y * cols
    keep = (row_at >= 0) & (row_at < rows * count_x) & (col_at >= 0) & (col_at < cols * count_y)
    keep = keep & (col_in >= -HALO)

    own = (
        [coef_ref[...]] + [force_ref[c] for c in range(3)] + [field_ref[c] for c in range(3)]
        if first
        else [field_ref[c] for c in range(3)] + [applied_ref[c] for c in range(3)]
    )
    count = len(own)
    base = HALO * count
    row_is_even, col_is_even = place_x % 2 == 0, place_y % 2 == 0
    even_in, odd_in = even_ref[...], odd_ref[...]
    side_left[0:rows, :] = jnp.where(col_is_even, odd_in, even_in)
    side_right[0:rows, :] = jnp.where(col_is_even, even_in, odd_in)
    even_in, odd_in = row_even_ref[...], row_odd_ref[...]
    from_down = jnp.where(row_is_even, even_in, odd_in)
    from_up = jnp.where(row_is_even, odd_in, even_in)
    side_left[rows : rows + HALO, :] = from_down[base : base + HALO]
    side_left[rows + HALO : tall, :] = from_up[base : base + HALO]
    side_right[rows : rows + HALO, :] = from_down[base + HALO : base + 2 * HALO]
    side_right[rows + HALO : tall, :] = from_up[base + HALO : base + 2 * HALO]
    lane = lanes_of((tall, cols))
    for k in range(count):
        ext[k, 0:rows, 0:cols] = own[k]
        ext[k, rows : rows + HALO, 0:cols] = from_down[HALO * k : HALO * (k + 1)]
        ext[k, rows + HALO : tall, 0:cols] = from_up[HALO * k : HALO * (k + 1)]
        close = side_right[...]
        close = pltpu.roll(close, cols - HALO * k, 1) if k else close
        far = pltpu.roll(side_left[...], cols - HALO * (k + 1), 1)
        ext[k, :, cols:wide] = jnp.where(lane < HALO, close, far)
        ext[k] = jnp.where(keep, ext[k], 0.0)
    if first:
        for k in range(4):
            static_out[k] = ext[k]
        at = 4
    else:
        at = 0

    def static(k):
        return ext[k] if first else static_ref[k]

    def load(c):
        return static(1 + c) if first else static(1 + c) + ext[3 + c]

    @pl.when(grp == 0)
    def _():
        nu = static(0)
        weights = [0.5 * (nu + move(nu)) for move in (below, above, right, left)]
        for k, w in enumerate(weights):
            node[k] = w
        for c in range(3):
            node[4 + c] = load(c)

        def flow(_, carry):
            for c in range(3):
                x = ext[at + c]
                total = node[4 + c]
                for k, move in enumerate((below, above, right, left)):
                    total = total + node[k] * (move(x) - x)
                ext[at + c] = jnp.where(keep, x + DT_STEP * total, 0.0)
            return carry

        lax.fori_loop(0, SUB, flow, 0)

    @pl.when(grp != 0)
    def _():
        kappa = static(0)
        kappa_up, kappa_left = above(kappa), left(kappa)
        kappa_both = left(kappa_up)
        for c in range(3):
            diagonal = (
                elem_ref[c, c] * kappa
                + elem_ref[3 + c, 3 + c] * kappa_up
                + elem_ref[6 + c, 6 + c] * kappa_left
                + elem_ref[9 + c, 9 + c] * kappa_both
            )
            diagonal = jnp.where(keep, diagonal, 1.0)
            node[12 + c] = jnp.where(keep, RELAX / diagonal, 0.0)
            node[15 + c] = load(c)

        def shell(_, carry):
            for c in range(3):
                x = ext[at + c]
                low = below(x)
                node[c] = x
                node[3 + c] = low
                node[6 + c] = right(x)
                node[9 + c] = right(low)

            def force(a):
                total = elem_ref[a, 0] * node[0]
                for b in range(1, 12):
                    total = total + elem_ref[a, b] * node[b]
                return total * static(0)

            for c in range(3):
                pull = force(c) + above(force(3 + c)) + left(force(6 + c) + above(force(9 + c)))
                ext[at + c] = ext[at + c] + node[12 + c] * (node[15 + c] - pull)
            return carry

        lax.fori_loop(0, SUB, shell, 0)

    for c in range(3):
        state_out[c] = ext[at + c, 0:rows, 0:cols]
    group = 8
    batch = min(PICK_BATCH, blocks // group)

    def pick(step, carry):
        for q in range(batch):
            start = pl.multiple_of((step * batch + q) * group, group)
            cell = source_ref[pl.ds(start, group), :]
            row_of, col_of = cell // cols, cell % cols
            found = [jnp.zeros((group, cols), jnp.float32) for _ in range(3)]
            for r in range(rows):
                here = row_of == r
                for c in range(3):
                    line = jnp.broadcast_to(ext[at + c, r : r + 1, 0:cols], (group, cols))
                    got = jnp.take_along_axis(line, col_of, axis=1)
                    found[c] = jnp.where(here, got, found[c])
            for c in range(3):
                reads[pl.ds(3 * start + c * group, group), :] = found[c]
        return carry

    lax.fori_loop(0, blocks // group // batch, pick, 0)
    fetch.wait()
    chunk = min(MAP_BATCH, blocks // group)
    block_id = lax.broadcasted_iota(jnp.int32, (3 * group, cols), 0) % group

    def send(step, carry):
        for q in range(chunk):
            start = pl.multiple_of((step * chunk + q) * group, group)
            read = reads[pl.ds(3 * start, 3 * group), :]
            for k in range(0, group, 2):
                halves = [jnp.where(block_id == k + h, read, 0.0).astype(jnp.bfloat16) for h in range(2)]
                matrix = map_ref[pl.ds(start + k, 2)].reshape(2 * cols, cols)
                mapped = jnp.dot(
                    jnp.concatenate(halves, axis=1), matrix, preferred_element_type=jnp.float32
                )
                for h in range(2):
                    place = slot_ref[start + k + h] * slot_rows
                    for c in range(3):
                        at_row = c * group + k + h
                        send_out[pl.ds(place + c, 1), :] = mapped[at_row : at_row + 1]
                    if first:
                        send_out[pl.ds(place + 3, 1), :] = target_ref[
                            pl.ds(start + k + h, 1), :
                        ].astype(jnp.float32)
        return carry

    lax.fori_loop(0, blocks // group // chunk, send, 0)


def scatter_kernel(arrived_ref, *refs, first, last, sizes, batch):
    rows, cols, slots = sizes
    refs = list(refs)
    place_ref = None if last else refs.pop(0)
    cells_ref = None if first else refs.pop(0)
    field_ref = None if last else refs.pop(0)
    applied_out = refs.pop(0)
    slot_rows = SLOT_ROWS if first else SLOT_ROWS - 1
    if first:
        cells_out = refs.pop(0)
        cells_out[...] = arrived_ref[pl.ds(SLOT_ROWS - 1, slots, stride=SLOT_ROWS), :].astype(jnp.int32)
        cells_ref = cells_out
    row_id = lax.broadcasted_iota(jnp.int32, (rows, cols), 0)
    col_id = lax.broadcasted_iota(jnp.int32, (cols, cols), 0)
    group = 8

    def add(step, total):
        spread, choose = [], []
        for part in range(batch // group):
            slot = pl.multiple_of(step * batch + part * group, group)
            cell = cells_ref[pl.ds(slot, group), :]
            cell_row, cell_col = cell // cols, cell % cols
            tile = arrived_ref[pl.ds(pl.multiple_of(slot * slot_rows, 8), group * slot_rows), :]
            for q in range(group):
                at = q * slot_rows
                here = row_id == cell_row[q : q + 1]
                spread.append(
                    jnp.concatenate(
                        [jnp.where(here, tile[at + c : at + c + 1], 0.0) for c in range(3)], axis=0
                    ).astype(jnp.bfloat16)
                )
                choose.append(
                    jnp.where(col_id == cell_col[q : q + 1], 1.0, 0.0).astype(jnp.bfloat16)
                )
        return total + lax.dot_general(
            jnp.concatenate(spread, axis=1),
            jnp.concatenate(choose, axis=1),
            (((1,), (1,)), ((), ())),
            preferred_element_type=jnp.float32,
        )

    total = lax.fori_loop(0, slots // batch, add, jnp.zeros((3 * rows, cols), jnp.float32))
    parts = [total[rows * c : rows * (c + 1)] for c in range(3)]
    for c in range(3):
        applied_out[c] = parts[c]
    if not last:
        pack_sides([field_ref[c] for c in range(3)] + parts, place_ref, *refs)


def body(
    fields,
    coefficients,
    forcing,
    element_matrix,
    source_cells,
    target_cells,
    peer_map,
    mapping_blocks,
):
    rows_x, rows_y = lax.axis_size("gx"), lax.axis_size("gy")
    state, coef, force = fields[0], coefficients[0], forcing[0]
    comps, rows, cols = state.shape
    blocks = peer_map.shape[1]
    partners = rows_x * rows_y
    slots = partners * CAPACITY
    tall, wide = rows + 2 * HALO, 2 * cols
    place = jnp.stack([lax.axis_index("grp"), lax.axis_index("gx"), lax.axis_index("gy")]).astype(
        jnp.int32
    )
    full = pltpu.VMEM((comps, rows, cols), jnp.float32)
    full_hbm = jax.ShapeDtypeStruct((comps, rows, cols), jnp.float32)
    kept = pltpu.VMEM((4, tall, wide), jnp.float32)
    grp_swap = [(0, 1), (1, 0)]

    packed = pl.pallas_call(
        first_pack_kernel,
        out_shape=pack_shapes(7, rows, cols),
        in_specs=[SMEM_SPEC] + [VMEM_SPEC] * 3,
        name="first_pack",
        interpret=INTERPRET,
    )(place, coef, force, state)
    slot_of, source, target = pl.pallas_call(
        prepare_kernel,
        out_shape=[
            jax.ShapeDtypeStruct((blocks,), jnp.int32),
            pltpu.VMEM((blocks, cols), jnp.int32),
            pltpu.VMEM((blocks, cols), jnp.int32),
        ],
        in_specs=[SMEM_SPEC] + [ANY_SPEC] * 2,
        out_specs=[SMEM_SPEC, VMEM_SPEC, VMEM_SPEC],
        scratch_shapes=[pltpu.SMEM((partners,), jnp.int32), pltpu.SemaphoreType.DMA((2,))],
        name="prepare",
        interpret=INTERPRET,
    )(peer_map[0, :, 0], source_cells[0], target_cells[0])
    applied, static, cells = None, None, None
    for outer in range(ITERS):
        first, last = outer == 0, outer == ITERS - 1
        sides = exchange(packed, place, *([slot_of] if first else []))
        slot_rows = SLOT_ROWS if first else SLOT_ROWS - 1
        wire = pltpu.VMEM((slots * slot_rows, cols), jnp.float32)
        lead = (coef, force, state) if first else (static, state, applied)
        swept = pl.pallas_call(
            lambda *refs, first=first: sweep_kernel(
                *refs, first=first, sizes=(rows, cols, blocks), count_x=rows_x, count_y=rows_y
            ),
            out_shape=[full_hbm if last else full, wire] + ([kept] if first else []),
            in_specs=[SMEM_SPEC] * 3 + [VMEM_SPEC] * 8 + [ANY_SPEC] + [VMEM_SPEC] * first,
            scratch_shapes=[
                pltpu.VMEM((7 if first else 6, tall, wide), jnp.float32),
                pltpu.VMEM((tall, cols), jnp.float32),
                pltpu.VMEM((tall, cols), jnp.float32),
                pltpu.VMEM((18, tall, wide), jnp.float32),
                pltpu.VMEM((blocks * 3, cols), jnp.float32),
                pltpu.VMEM(mapping_blocks.shape[1:], jnp.bfloat16),
                pltpu.SemaphoreType.DMA,
            ],
            name="sweep_first" if first else "sweep",
            interpret=INTERPRET,
        )(
            place,
            slot_of,
            element_matrix,
            *(lead if first else map(near, lead)),
            *map(near, sides),
            near(source),
            mapping_blocks[0],
            *([near(target)] if first else []),
        )
        if first:
            state, send, static = swept
        else:
            state, send = swept
        crossed = lax.ppermute(send, "grp", grp_swap)
        arrived = lax.all_to_all(
            crossed.reshape((partners, CAPACITY * SLOT_ROWS, cols) if first else (partners, 3, CAPACITY, cols)),
            ("gx", "gy"),
            split_axis=0,
            concat_axis=0,
            tiled=True,
        ).reshape(slots * slot_rows, cols)
        received = pl.pallas_call(
            lambda *refs, first=first, last=last: scatter_kernel(
                *refs, first=first, last=last, sizes=(rows, cols, slots), batch=min(SCATTER_BATCH, slots)
            ),
            out_shape=[full_hbm if last else full]
            + ([pltpu.VMEM((slots, cols), jnp.int32)] if first else [])
            + ([] if last else pack_shapes(6, rows, cols)),
            in_specs=[VMEM_SPEC] + [SMEM_SPEC] * (not last) + [VMEM_SPEC] * (2 - first - last),
            name="scatter_first" if first else "scatter_last" if last else "scatter",
            interpret=INTERPRET,
        )(
            near(arrived),
            *([] if last else [place]),
            *([] if first else [near(cells)]),
            *([] if last else [near(state)]),
        )
        applied, packed = received[0], received[1:]
        if first:
            cells, packed = packed[0], packed[1:]
    return (state[None], applied[None])


def solution(mesh):
    placed = (
        P("grp", None, "gx", "gy"),
        P("grp", "gx", "gy"),
        P("grp", None, "gx", "gy"),
        P(),
        P("grp", ("gx", "gy"), None),
        P("grp", ("gx", "gy"), None),
        P("grp", ("gx", "gy"), None),
        P("grp", ("gx", "gy"), None, None),
    )
    return jax.shard_map(
        body,
        mesh=mesh,
        in_specs=placed,
        out_specs=(P("grp", None, "gx", "gy"), P("grp", None, "gx", "gy")),
        check_vma=False,
    )
```

```python
import jax
import jax.numpy as jnp
from jax import lax
from jax.experimental import pallas as pl
from jax.experimental.pallas import tpu as pltpu
from jax.sharding import PartitionSpec as P

ITERS = 4
SUB = 4
HALO = 4
DT_STEP = 1.0
RELAX = 0.6
SLOT_ROWS = 4
SCALARS = 128
CAPACITY = 2
PICK_BATCH = 4
MAP_BATCH = 8
SCATTER_BATCH = 128

INTERPRET = False

VMEM_SPEC = pl.BlockSpec(memory_space=pltpu.VMEM)
ANY_SPEC = pl.BlockSpec(memory_space=pl.ANY)
SMEM_SPEC = pl.BlockSpec(memory_space=pltpu.SMEM)


def near(x):
    return x if INTERPRET else pltpu.with_memory_space_constraint(x, pltpu.VMEM)


def lanes_of(shape):
    return lax.broadcasted_iota(jnp.int32, shape, len(shape) - 1)


def below(x):
    return pltpu.roll(x, x.shape[0] - 1, 0)


def above(x):
    return pltpu.roll(x, 1, 0)


def right(x):
    return pltpu.roll(x, x.shape[1] - 1, 1)


def left(x):
    return pltpu.roll(x, 1, 1)


def row_parity(flag_ref, shape):
    return jnp.broadcast_to(flag_ref[0:1, :], shape) == 0


def col_parity(flag_ref, shape):
    return jnp.broadcast_to(flag_ref[8:9, :], shape) == 0


def pack_sides(parts, flag_ref, even_out, odd_out, top_out, bottom_out):
    rows, cols = parts[0].shape
    lane = lanes_of((rows, cols))
    low = jnp.zeros((rows, cols), jnp.float32)
    high = low
    for k, x in enumerate(parts):
        here = (lane >= HALO * k) & (lane < HALO * (k + 1))
        low = jnp.where(here, pltpu.roll(x, HALO * k, 1) if k else x, low)
        high = jnp.where(here, pltpu.roll(x, HALO * (k + 1), 1), high)
        top_out[HALO * k : HALO * (k + 1), :] = x[:HALO]
        bottom_out[HALO * k : HALO * (k + 1), :] = x[rows - HALO :]
    is_even = col_parity(flag_ref, (rows, cols))
    even_out[...] = jnp.where(is_even, high, low)
    odd_out[...] = jnp.where(is_even, low, high)


def first_pack_kernel(flag_ref, coef_ref, force_ref, field_ref, flag_out, *outs):
    flag_out[...] = flag_ref[...]
    parts = [coef_ref[...]] + [force_ref[c] for c in range(3)] + [field_ref[c] for c in range(3)]
    pack_sides(parts, flag_ref, *outs)


def pack_shapes(count, rows, cols):
    side = pltpu.VMEM((rows, cols), jnp.float32)
    ends = pltpu.VMEM((HALO * count, cols), jnp.float32)
    return [side, side, ends, ends]


def prepare_kernel(
    peer_ref, source_hbm, target_hbm, slot_out, source_out, target_out, seen, sems
):
    fetches = [
        pltpu.make_async_copy(source, target, sems.at[k])
        for k, (source, target) in enumerate(
            ((source_hbm, source_out), (target_hbm, target_out))
        )
    ]
    for fetch in fetches:
        fetch.start()

    def clear(i, carry):
        seen[i] = 0
        return carry

    lax.fori_loop(0, seen.shape[0], clear, 0, unroll=16)

    def place(i, carry):
        peer = peer_ref[i]
        rank = seen[peer]
        slot_out[i] = peer * CAPACITY + rank
        seen[peer] = rank + 1
        return carry

    lax.fori_loop(0, peer_ref.shape[0], place, 0, unroll=8)
    for fetch in fetches:
        fetch.wait()


def edge_kernel(flag_ref, top_ref, bottom_ref, even_ref, odd_ref, odd_out, even_out):
    base, (rows, cols) = top_ref.shape[0], even_ref.shape
    col_even = col_parity(flag_ref, (rows, cols))
    even_in, odd_in = even_ref[...], odd_ref[...]
    from_left = jnp.where(col_even, odd_in, even_in)
    from_right = jnp.where(col_even, even_in, odd_in)

    def put(start, upper, lower):
        row_even = row_parity(flag_ref, upper.shape)
        stop = start + upper.shape[0]
        even_out[start:stop, :] = jnp.where(row_even, lower, upper)
        odd_out[start:stop, :] = jnp.where(row_even, upper, lower)

    put(0, top_ref[...], bottom_ref[...])
    put(base, from_left[:HALO], from_left[rows - HALO :])
    put(base + HALO, from_right[:HALO], from_right[rows - HALO :])


def swap_even(value, axis):
    return lax.ppermute(value, axis, [(i, i ^ 1) for i in range(lax.axis_size(axis))])


def swap_odd(value, axis):
    count = lax.axis_size(axis)
    return lax.ppermute(value, axis, [(i, (((i + 1) ^ 1) - 1) % count) for i in range(count)])


def exchange(packed, flags):
    even, odd, top, bottom = packed
    even, odd = swap_even(even, "gy"), swap_odd(odd, "gy")
    ends = pltpu.VMEM((top.shape[0] + 2 * HALO, top.shape[1]), jnp.float32)
    row_odd, row_even = pl.pallas_call(
        edge_kernel, out_shape=[ends, ends], name="edges", interpret=INTERPRET
    )(near(flags), near(top), near(bottom), near(even), near(odd))
    row_odd = swap_odd(row_odd, "gx")
    row_even = swap_even(row_even, "gx")
    return even, odd, row_even, row_odd


def sweep_kernel(*refs, first, sizes, count_x, count_y):
    rows, cols, blocks = sizes
    tall, wide = rows + 2 * HALO, 2 * cols
    scalars, flag_ref = refs[:3], refs[3]
    if first:
        coef_ref, force_ref, field_ref = refs[4:7]
    else:
        static_ref, field_ref, applied_ref = refs[4:7]
    even_ref, odd_ref, row_even_ref, row_odd_ref, source_ref, map_hbm = refs[7:13]
    if first:
        target_ref = refs[13]
    outs = refs[14:] if first else refs[13:]
    slot_rows = SLOT_ROWS if first else SLOT_ROWS - 1
    if first:
        state_out, send_out, static_out = outs[:3]
        scratch = outs[3:]
    else:
        state_out, send_out = outs[:2]
        scratch = outs[2:]
    ext, side_left, side_right, node, reads, map_ref, place_ref, slot_ref, elem_ref, sems = scratch
    small = [
        pltpu.make_async_copy(source, target, sems.at[k])
        for k, (source, target) in enumerate(zip(scalars, (place_ref, slot_ref, elem_ref)))
    ]
    fetch = pltpu.make_async_copy(map_hbm, map_ref, sems.at[3])
    for copy in small:
        copy.start()
    fetch.start()
    send_out[...] = jnp.zeros(send_out.shape, jnp.float32)

    if first:
        small[0].wait()
        place_x, place_y = place_ref[1], place_ref[2]
        row_id = lax.broadcasted_iota(jnp.int32, (tall, wide), 0)
        col_id = lax.broadcasted_iota(jnp.int32, (tall, wide), 1)
        row_at = jnp.where(row_id < rows + HALO, row_id, row_id - tall) + place_x * rows
        col_in = jnp.where(col_id < cols + HALO, col_id, col_id - wide)
        col_at = col_in + place_y * cols
        keep = (row_at >= 0) & (row_at < rows * count_x) & (col_at >= 0) & (col_at < cols * count_y)
        keep = keep & (col_in >= -HALO)
    else:
        keep = static_ref[4] > 0.5

    own = (
        [coef_ref[...]] + [force_ref[c] for c in range(3)] + [field_ref[c] for c in range(3)]
        if first
        else [field_ref[c] for c in range(3)] + [applied_ref[c] for c in range(3)]
    )
    count = len(own)
    base = HALO * count
    col_is_even = col_parity(flag_ref, even_ref.shape)
    row_is_even = row_parity(flag_ref, row_even_ref.shape)
    even_in, odd_in = even_ref[...], odd_ref[...]
    side_left[0:rows, :] = jnp.where(col_is_even, odd_in, even_in)
    side_right[0:rows, :] = jnp.where(col_is_even, even_in, odd_in)
    even_in, odd_in = row_even_ref[...], row_odd_ref[...]
    from_down = jnp.where(row_is_even, even_in, odd_in)
    from_up = jnp.where(row_is_even, odd_in, even_in)
    side_left[rows : rows + HALO, :] = from_down[base : base + HALO]
    side_left[rows + HALO : tall, :] = from_up[base : base + HALO]
    side_right[rows : rows + HALO, :] = from_down[base + HALO : base + 2 * HALO]
    side_right[rows + HALO : tall, :] = from_up[base + HALO : base + 2 * HALO]
    lane = lanes_of((tall, cols))
    for k in range(count):
        ext[k, 0:rows, 0:cols] = own[k]
        ext[k, rows : rows + HALO, 0:cols] = from_down[HALO * k : HALO * (k + 1)]
        ext[k, rows + HALO : tall, 0:cols] = from_up[HALO * k : HALO * (k + 1)]
        close = side_right[...]
        close = pltpu.roll(close, cols - HALO * k, 1) if k else close
        far = pltpu.roll(side_left[...], cols - HALO * (k + 1), 1)
        ext[k, :, cols:wide] = jnp.where(lane < HALO, close, far)
        ext[k] = jnp.where(keep, ext[k], 0.0)
    if first:
        for k in range(4):
            static_out[k] = ext[k]
        static_out[4] = jnp.where(keep, 1.0, 0.0)
        at = 4
    else:
        at = 0

    def static(k):
        return ext[k] if first else static_ref[k]

    def load(c):
        return static(1 + c) if first else static(1 + c) + ext[3 + c]

    for copy in small[1:] if first else small:
        copy.wait()
    grp = place_ref[0]

    @pl.when(grp == 0)
    def _():
        nu = static(0)
        weights = [0.5 * (nu + move(nu)) for move in (below, above, right, left)]
        for k, w in enumerate(weights):
            node[k] = w
        for c in range(3):
            node[4 + c] = load(c)

        def flow(_, carry):
            for c in range(3):
                x = ext[at + c]
                total = node[4 + c]
                for k, move in enumerate((below, above, right, left)):
                    total = total + node[k] * (move(x) - x)
                ext[at + c] = jnp.where(keep, x + DT_STEP * total, 0.0)
            return carry

        lax.fori_loop(0, SUB, flow, 0)

    @pl.when(grp != 0)
    def _():
        kappa = static(0)
        kappa_up, kappa_left = above(kappa), left(kappa)
        kappa_both = left(kappa_up)
        for c in range(3):
            diagonal = (
                elem_ref[13 * c] * kappa
                + elem_ref[39 + 13 * c] * kappa_up
                + elem_ref[78 + 13 * c] * kappa_left
                + elem_ref[117 + 13 * c] * kappa_both
            )
            diagonal = jnp.where(keep, diagonal, 1.0)
            node[12 + c] = jnp.where(keep, RELAX / diagonal, 0.0)
            node[15 + c] = load(c)

        def shell(_, carry):
            for c in range(3):
                x = ext[at + c]
                low = below(x)
                node[c] = x
                node[3 + c] = low
                node[6 + c] = right(x)
                node[9 + c] = right(low)

            def force(a):
                total = elem_ref[12 * a] * node[0]
                for b in range(1, 12):
                    total = total + elem_ref[12 * a + b] * node[b]
                return total * static(0)

            for c in range(3):
                pull = force(c) + above(force(3 + c)) + left(force(6 + c) + above(force(9 + c)))
                ext[at + c] = ext[at + c] + node[12 + c] * (node[15 + c] - pull)
            return carry

        lax.fori_loop(0, SUB, shell, 0)

    for c in range(3):
        state_out[c] = ext[at + c, 0:rows, 0:cols]
    group = 8
    batch = min(PICK_BATCH, blocks // group)

    def pick(step, carry):
        for q in range(batch):
            start = pl.multiple_of((step * batch + q) * group, group)
            cell = source_ref[pl.ds(start, group), :]
            row_of, col_of = cell // cols, cell % cols
            found = [jnp.zeros((group, cols), jnp.float32) for _ in range(3)]
            for r in range(rows):
                here = row_of == r
                for c in range(3):
                    line = jnp.broadcast_to(ext[at + c, r : r + 1, 0:cols], (group, cols))
                    got = jnp.take_along_axis(line, col_of, axis=1)
                    found[c] = jnp.where(here, got, found[c])
            for c in range(3):
                reads[pl.ds(3 * start + c * group, group), :] = found[c]
        return carry

    lax.fori_loop(0, blocks // group // batch, pick, 0)
    fetch.wait()
    chunk = min(MAP_BATCH, blocks // group)
    block_id = lax.broadcasted_iota(jnp.int32, (3 * group, cols), 0) % group

    def send(step, carry):
        for q in range(chunk):
            start = pl.multiple_of((step * chunk + q) * group, group)
            read = reads[pl.ds(3 * start, 3 * group), :]
            for k in range(0, group, 2):
                halves = [jnp.where(block_id == k + h, read, 0.0).astype(jnp.bfloat16) for h in range(2)]
                matrix = map_ref[pl.ds(start + k, 2)].reshape(2 * cols, cols)
                mapped = jnp.dot(
                    jnp.concatenate(halves, axis=1), matrix, preferred_element_type=jnp.float32
                )
                for h in range(2):
                    place = slot_ref[start + k + h] * slot_rows
                    for c in range(3):
                        at_row = c * group + k + h
                        send_out[pl.ds(place + c, 1), :] = mapped[at_row : at_row + 1]
                    if first:
                        send_out[pl.ds(place + 3, 1), :] = target_ref[
                            pl.ds(start + k + h, 1), :
                        ].astype(jnp.float32)
        return carry

    lax.fori_loop(0, blocks // group // chunk, send, 0)


def scatter_kernel(arrived_ref, *refs, first, last, sizes, batch):
    rows, cols, slots = sizes
    refs = list(refs)
    flag_ref = None if last else refs.pop(0)
    cells_ref = None if first else refs.pop(0)
    field_ref = None if last else refs.pop(0)
    applied_out = refs.pop(0)
    slot_rows = SLOT_ROWS if first else SLOT_ROWS - 1
    if first:
        cells_out = refs.pop(0)
        cells_out[...] = arrived_ref[pl.ds(SLOT_ROWS - 1, slots, stride=SLOT_ROWS), :].astype(jnp.int32)
        cells_ref = cells_out
    row_id = lax.broadcasted_iota(jnp.int32, (rows, cols), 0)
    col_id = lax.broadcasted_iota(jnp.int32, (cols, cols), 0)
    group = 8

    def add(step, total):
        spread, choose = [], []
        for part in range(batch // group):
            slot = pl.multiple_of(step * batch + part * group, group)
            cell = cells_ref[pl.ds(slot, group), :]
            cell_row, cell_col = cell // cols, cell % cols
            tile = arrived_ref[pl.ds(pl.multiple_of(slot * slot_rows, 8), group * slot_rows), :]
            for q in range(group):
                at = q * slot_rows
                here = row_id == cell_row[q : q + 1]
                spread.append(
                    jnp.concatenate(
                        [jnp.where(here, tile[at + c : at + c + 1], 0.0) for c in range(3)], axis=0
                    ).astype(jnp.bfloat16)
                )
                choose.append(
                    jnp.where(col_id == cell_col[q : q + 1], 1.0, 0.0).astype(jnp.bfloat16)
                )
        return total + lax.dot_general(
            jnp.concatenate(spread, axis=1),
            jnp.concatenate(choose, axis=1),
            (((1,), (1,)), ((), ())),
            preferred_element_type=jnp.float32,
        )

    total = lax.fori_loop(0, slots // batch, add, jnp.zeros((3 * rows, cols), jnp.float32))
    parts = [total[rows * c : rows * (c + 1)] for c in range(3)]
    for c in range(3):
        applied_out[c] = parts[c]
    if not last:
        pack_sides([field_ref[c] for c in range(3)] + parts, flag_ref, *refs)


def body(
    fields,
    coefficients,
    forcing,
    element_matrix,
    source_cells,
    target_cells,
    peer_map,
    mapping_blocks,
):
    rows_x, rows_y = lax.axis_size("gx"), lax.axis_size("gy")
    state, coef, force = fields[0], coefficients[0], forcing[0]
    comps, rows, cols = state.shape
    blocks = peer_map.shape[1]
    partners = rows_x * rows_y
    slots = partners * CAPACITY
    tall, wide = rows + 2 * HALO, 2 * cols
    place_x, place_y = lax.axis_index("gx"), lax.axis_index("gy")
    place = jnp.pad(
        jnp.stack([lax.axis_index("grp"), place_x, place_y]).astype(jnp.int32), (0, SCALARS - 3)
    )
    upper = lax.broadcasted_iota(jnp.int32, (16, cols), 0) < 8
    flags = jnp.where(upper, place_x % 2, place_y % 2).astype(jnp.int32)
    elements = jnp.pad(element_matrix.reshape(-1), (0, 2 * SCALARS - 144))
    full = pltpu.VMEM((comps, rows, cols), jnp.float32)
    full_hbm = jax.ShapeDtypeStruct((comps, rows, cols), jnp.float32)
    kept = pltpu.VMEM((5, tall, wide), jnp.float32)
    grp_swap = [(0, 1), (1, 0)]

    flags, *packed = pl.pallas_call(
        first_pack_kernel,
        out_shape=[pltpu.VMEM(flags.shape, jnp.int32)] + pack_shapes(7, rows, cols),
        name="first_pack",
        interpret=INTERPRET,
    )(flags, coef, force, state)
    slot_of, source, target = pl.pallas_call(
        prepare_kernel,
        out_shape=[
            jax.ShapeDtypeStruct((SCALARS,), jnp.int32),
            pltpu.VMEM((blocks, cols), jnp.int32),
            pltpu.VMEM((blocks, cols), jnp.int32),
        ],
        in_specs=[SMEM_SPEC] + [ANY_SPEC] * 2,
        out_specs=[SMEM_SPEC, VMEM_SPEC, VMEM_SPEC],
        scratch_shapes=[pltpu.SMEM((partners,), jnp.int32), pltpu.SemaphoreType.DMA((2,))],
        name="prepare",
        interpret=INTERPRET,
    )(peer_map[0, :, 0], source_cells[0], target_cells[0])
    applied, static, cells = None, None, None
    for outer in range(ITERS):
        first, last = outer == 0, outer == ITERS - 1
        sides = exchange(packed, flags)
        slot_rows = SLOT_ROWS if first else SLOT_ROWS - 1
        wire = pltpu.VMEM((slots * slot_rows, cols), jnp.float32)
        lead = (coef, force, state) if first else (static, state, applied)
        swept = pl.pallas_call(
            lambda *refs, first=first: sweep_kernel(
                *refs, first=first, sizes=(rows, cols, blocks), count_x=rows_x, count_y=rows_y
            ),
            out_shape=[full_hbm if last else full, wire] + ([kept] if first else []),
            in_specs=[ANY_SPEC] * 3 + [VMEM_SPEC] * 9 + [ANY_SPEC] + [VMEM_SPEC] * first,
            scratch_shapes=[
                pltpu.VMEM((7 if first else 6, tall, wide), jnp.float32),
                pltpu.VMEM((tall, cols), jnp.float32),
                pltpu.VMEM((tall, cols), jnp.float32),
                pltpu.VMEM((18, tall, wide), jnp.float32),
                pltpu.VMEM((blocks * 3, cols), jnp.float32),
                pltpu.VMEM(mapping_blocks.shape[1:], jnp.bfloat16),
                pltpu.SMEM((SCALARS,), jnp.int32),
                pltpu.SMEM((SCALARS,), jnp.int32),
                pltpu.SMEM((2 * SCALARS,), jnp.float32),
                pltpu.SemaphoreType.DMA((4,)),
            ],
            name="sweep_first" if first else "sweep",
            interpret=INTERPRET,
        )(
            place,
            slot_of,
            elements,
            near(flags),
            *(lead if first else map(near, lead)),
            *map(near, sides),
            near(source),
            mapping_blocks[0],
            *([near(target)] if first else []),
        )
        if first:
            state, send, static = swept
        else:
            state, send = swept
        crossed = lax.ppermute(send, "grp", grp_swap)
        arrived = lax.all_to_all(
            crossed.reshape((partners, CAPACITY * SLOT_ROWS, cols) if first else (partners, 3, CAPACITY, cols)),
            ("gx", "gy"),
            split_axis=0,
            concat_axis=0,
            tiled=True,
        ).reshape(slots * slot_rows, cols)
        received = pl.pallas_call(
            lambda *refs, first=first, last=last: scatter_kernel(
                *refs, first=first, last=last, sizes=(rows, cols, slots), batch=min(SCATTER_BATCH, slots)
            ),
            out_shape=[full_hbm if last else full]
            + ([pltpu.VMEM((slots, cols), jnp.int32)] if first else [])
            + ([] if last else pack_shapes(6, rows, cols)),
            name="scatter_first" if first else "scatter_last" if last else "scatter",
            interpret=INTERPRET,
        )(
            near(arrived),
            *([] if last else [near(flags)]),
            *([] if first else [near(cells)]),
            *([] if last else [near(state)]),
        )
        applied, packed = received[0], received[1:]
        if first:
            cells, packed = packed[0], packed[1:]
    return (state[None], applied[None])


def solution(mesh):
    placed = (
        P("grp", None, "gx", "gy"),
        P("grp", "gx", "gy"),
        P("grp", None, "gx", "gy"),
        P(),
        P("grp", ("gx", "gy"), None),
        P("grp", ("gx", "gy"), None),
        P("grp", ("gx", "gy"), None),
        P("grp", ("gx", "gy"), None, None),
    )
    return jax.shard_map(
        body,
        mesh=mesh,
        in_specs=placed,
        out_specs=(P("grp", None, "gx", "gy"), P("grp", None, "gx", "gy")),
        check_vma=False,
    )
```

```python
import jax
import jax.numpy as jnp
from jax import lax
from jax.experimental import pallas as pl
from jax.experimental.pallas import tpu as pltpu
from jax.sharding import PartitionSpec as P

ITERS = 4
SUB = 4
HALO = 4
DT_STEP = 1.0
RELAX = 0.6
SLOT_ROWS = 4
SCALARS = 128
CAPACITY = 2
PICK_BATCH = 4
MAP_BATCH = 8
SCATTER_BATCH = 256

INTERPRET = False

VMEM_SPEC = pl.BlockSpec(memory_space=pltpu.VMEM)
ANY_SPEC = pl.BlockSpec(memory_space=pl.ANY)
SMEM_SPEC = pl.BlockSpec(memory_space=pltpu.SMEM)


def near(x):
    return x if INTERPRET else pltpu.with_memory_space_constraint(x, pltpu.VMEM)


def lanes_of(shape):
    return lax.broadcasted_iota(jnp.int32, shape, len(shape) - 1)


def below(x):
    return pltpu.roll(x, x.shape[0] - 1, 0)


def above(x):
    return pltpu.roll(x, 1, 0)


def right(x):
    return pltpu.roll(x, x.shape[1] - 1, 1)


def left(x):
    return pltpu.roll(x, 1, 1)


def row_parity(flag_ref, shape):
    return jnp.broadcast_to(flag_ref[0:1, :], shape) == 0


def col_parity(flag_ref, shape):
    return jnp.broadcast_to(flag_ref[8:9, :], shape) == 0


def pack_sides(parts, flag_ref, even_out, odd_out, top_out, bottom_out):
    rows, cols = parts[0].shape
    lane = lanes_of((rows, cols))
    low = jnp.zeros((rows, cols), jnp.float32)
    high = low
    for k, x in enumerate(parts):
        here = (lane >= HALO * k) & (lane < HALO * (k + 1))
        low = jnp.where(here, pltpu.roll(x, HALO * k, 1) if k else x, low)
        high = jnp.where(here, pltpu.roll(x, HALO * (k + 1), 1), high)
        top_out[HALO * k : HALO * (k + 1), :] = x[:HALO]
        bottom_out[HALO * k : HALO * (k + 1), :] = x[rows - HALO :]
    is_even = col_parity(flag_ref, (rows, cols))
    even_out[...] = jnp.where(is_even, high, low)
    odd_out[...] = jnp.where(is_even, low, high)


def first_pack_kernel(flag_ref, coef_ref, force_ref, field_ref, flag_out, *outs):
    flag_out[...] = flag_ref[...]
    parts = [coef_ref[...]] + [force_ref[c] for c in range(3)] + [field_ref[c] for c in range(3)]
    pack_sides(parts, flag_ref, *outs)


def pack_shapes(count, rows, cols):
    side = pltpu.VMEM((rows, cols), jnp.float32)
    ends = pltpu.VMEM((HALO * count, cols), jnp.float32)
    return [side, side, ends, ends]


def prepare_kernel(
    peer_ref, source_hbm, target_hbm, slot_out, source_out, target_out, seen, sems
):
    fetches = [
        pltpu.make_async_copy(source, target, sems.at[k])
        for k, (source, target) in enumerate(
            ((source_hbm, source_out), (target_hbm, target_out))
        )
    ]
    for fetch in fetches:
        fetch.start()

    def clear(i, carry):
        seen[i] = 0
        return carry

    lax.fori_loop(0, seen.shape[0], clear, 0, unroll=16)

    def place(i, carry):
        peer = peer_ref[i]
        rank = seen[peer]
        slot_out[i] = peer * CAPACITY + rank
        seen[peer] = rank + 1
        return carry

    lax.fori_loop(0, peer_ref.shape[0], place, 0, unroll=8)
    for fetch in fetches:
        fetch.wait()


def edge_kernel(flag_ref, top_ref, bottom_ref, even_ref, odd_ref, odd_out, even_out):
    base, (rows, cols) = top_ref.shape[0], even_ref.shape
    col_even = col_parity(flag_ref, (rows, cols))
    even_in, odd_in = even_ref[...], odd_ref[...]
    from_left = jnp.where(col_even, odd_in, even_in)
    from_right = jnp.where(col_even, even_in, odd_in)

    def put(start, upper, lower):
        row_even = row_parity(flag_ref, upper.shape)
        stop = start + upper.shape[0]
        even_out[start:stop, :] = jnp.where(row_even, lower, upper)
        odd_out[start:stop, :] = jnp.where(row_even, upper, lower)

    put(0, top_ref[...], bottom_ref[...])
    put(base, from_left[:HALO], from_left[rows - HALO :])
    put(base + HALO, from_right[:HALO], from_right[rows - HALO :])


def swap_even(value, axis):
    return lax.ppermute(value, axis, [(i, i ^ 1) for i in range(lax.axis_size(axis))])


def swap_odd(value, axis):
    count = lax.axis_size(axis)
    return lax.ppermute(value, axis, [(i, (((i + 1) ^ 1) - 1) % count) for i in range(count)])


def exchange(packed, flags):
    even, odd, top, bottom = packed
    even, odd = swap_even(even, "gy"), swap_odd(odd, "gy")
    ends = pltpu.VMEM((top.shape[0] + 2 * HALO, top.shape[1]), jnp.float32)
    row_odd, row_even = pl.pallas_call(
        edge_kernel, out_shape=[ends, ends], name="edges", interpret=INTERPRET
    )(near(flags), near(top), near(bottom), near(even), near(odd))
    row_odd = swap_odd(row_odd, "gx")
    row_even = swap_even(row_even, "gx")
    return even, odd, row_odd, row_even


def sweep_kernel(*refs, first, sizes, count_x, count_y):
    rows, cols, blocks = sizes
    tall, wide = rows + 2 * HALO, 2 * cols
    scalars, flag_ref = refs[:3], refs[3]
    if first:
        coef_ref, force_ref, field_ref = refs[4:7]
    else:
        static_ref, field_ref, applied_ref = refs[4:7]
    even_ref, odd_ref, row_odd_ref, row_even_ref, source_ref, map_hbm = refs[7:13]
    if first:
        target_ref = refs[13]
    outs = refs[14:] if first else refs[13:]
    slot_rows = SLOT_ROWS if first else SLOT_ROWS - 1
    if first:
        state_out, send_out, static_out = outs[:3]
        scratch = outs[3:]
    else:
        state_out, send_out = outs[:2]
        scratch = outs[2:]
    ext, side_left, side_right, node, reads, map_ref, place_ref, slot_ref, elem_ref, sems = scratch
    small = [
        pltpu.make_async_copy(source, target, sems.at[k])
        for k, (source, target) in enumerate(zip(scalars, (place_ref, slot_ref, elem_ref)))
    ]
    fetch = pltpu.make_async_copy(map_hbm, map_ref, sems.at[3])
    for copy in small:
        copy.start()
    fetch.start()
    send_out[...] = jnp.zeros(send_out.shape, jnp.float32)

    if first:
        small[0].wait()
        place_x, place_y = place_ref[1], place_ref[2]
        row_id = lax.broadcasted_iota(jnp.int32, (tall, wide), 0)
        col_id = lax.broadcasted_iota(jnp.int32, (tall, wide), 1)
        row_at = jnp.where(row_id < rows + HALO, row_id, row_id - tall) + place_x * rows
        col_in = jnp.where(col_id < cols + HALO, col_id, col_id - wide)
        col_at = col_in + place_y * cols
        keep = (row_at >= 0) & (row_at < rows * count_x) & (col_at >= 0) & (col_at < cols * count_y)
        keep = keep & (col_in >= -HALO)
    else:
        keep = static_ref[4] > 0.5

    own = (
        [coef_ref[...]] + [force_ref[c] for c in range(3)] + [field_ref[c] for c in range(3)]
        if first
        else [field_ref[c] for c in range(3)] + [applied_ref[c] for c in range(3)]
    )
    count = len(own)
    base = HALO * count
    col_is_even = col_parity(flag_ref, even_ref.shape)
    row_is_even = row_parity(flag_ref, row_even_ref.shape)
    even_in, odd_in = even_ref[...], odd_ref[...]
    side_left[0:rows, :] = jnp.where(col_is_even, odd_in, even_in)
    side_right[0:rows, :] = jnp.where(col_is_even, even_in, odd_in)
    even_in, odd_in = row_even_ref[...], row_odd_ref[...]
    from_down = jnp.where(row_is_even, even_in, odd_in)
    from_up = jnp.where(row_is_even, odd_in, even_in)
    side_left[rows : rows + HALO, :] = from_down[base : base + HALO]
    side_left[rows + HALO : tall, :] = from_up[base : base + HALO]
    side_right[rows : rows + HALO, :] = from_down[base + HALO : base + 2 * HALO]
    side_right[rows + HALO : tall, :] = from_up[base + HALO : base + 2 * HALO]
    lane = lanes_of((tall, cols))
    for k in range(count):
        ext[k, 0:rows, 0:cols] = own[k]
        ext[k, rows : rows + HALO, 0:cols] = from_down[HALO * k : HALO * (k + 1)]
        ext[k, rows + HALO : tall, 0:cols] = from_up[HALO * k : HALO * (k + 1)]
        close = side_right[...]
        close = pltpu.roll(close, cols - HALO * k, 1) if k else close
        far = pltpu.roll(side_left[...], cols - HALO * (k + 1), 1)
        ext[k, :, cols:wide] = jnp.where(lane < HALO, close, far)
        ext[k] = jnp.where(keep, ext[k], 0.0)
    if first:
        for k in range(4):
            static_out[k] = ext[k]
        static_out[4] = jnp.where(keep, 1.0, 0.0)
        at = 4
    else:
        at = 0

    def static(k):
        return ext[k] if first else static_ref[k]

    def load(c):
        return static(1 + c) if first else static(1 + c) + ext[3 + c]

    for copy in small[1:] if first else small:
        copy.wait()
    grp = place_ref[0]

    @pl.when(grp == 0)
    def _():
        nu = static(0)
        weights = [0.5 * (nu + move(nu)) for move in (below, above, right, left)]
        for k, w in enumerate(weights):
            node[k] = w
        for c in range(3):
            node[4 + c] = load(c)

        def flow(_, carry):
            for c in range(3):
                x = ext[at + c]
                total = node[4 + c]
                for k, move in enumerate((below, above, right, left)):
                    total = total + node[k] * (move(x) - x)
                ext[at + c] = jnp.where(keep, x + DT_STEP * total, 0.0)
            return carry

        lax.fori_loop(0, SUB, flow, 0)

    @pl.when(grp != 0)
    def _():
        kappa = static(0)
        kappa_up, kappa_left = above(kappa), left(kappa)
        kappa_both = left(kappa_up)
        for c in range(3):
            diagonal = (
                elem_ref[13 * c] * kappa
                + elem_ref[39 + 13 * c] * kappa_up
                + elem_ref[78 + 13 * c] * kappa_left
                + elem_ref[117 + 13 * c] * kappa_both
            )
            diagonal = jnp.where(keep, diagonal, 1.0)
            node[12 + c] = jnp.where(keep, RELAX / diagonal, 0.0)
            node[15 + c] = load(c)

        def shell(_, carry):
            for c in range(3):
                x = ext[at + c]
                low = below(x)
                node[c] = x
                node[3 + c] = low
                node[6 + c] = right(x)
                node[9 + c] = right(low)

            def force(a):
                total = elem_ref[12 * a] * node[0]
                for b in range(1, 12):
                    total = total + elem_ref[12 * a + b] * node[b]
                return total * static(0)

            for c in range(3):
                pull = force(c) + above(force(3 + c)) + left(force(6 + c) + above(force(9 + c)))
                ext[at + c] = ext[at + c] + node[12 + c] * (node[15 + c] - pull)
            return carry

        lax.fori_loop(0, SUB, shell, 0)

    for c in range(3):
        state_out[c] = ext[at + c, 0:rows, 0:cols]
    group = 8
    batch = min(PICK_BATCH, blocks // group)

    def pick(step, carry):
        for q in range(batch):
            start = pl.multiple_of((step * batch + q) * group, group)
            cell = source_ref[pl.ds(start, group), :]
            row_of, col_of = cell // cols, cell % cols
            found = [jnp.zeros((group, cols), jnp.float32) for _ in range(3)]
            for r in range(rows):
                here = row_of == r
                for c in range(3):
                    line = jnp.broadcast_to(ext[at + c, r : r + 1, 0:cols], (group, cols))
                    got = jnp.take_along_axis(line, col_of, axis=1)
                    found[c] = jnp.where(here, got, found[c])
            for c in range(3):
                reads[pl.ds(3 * start + c * group, group), :] = found[c]
        return carry

    lax.fori_loop(0, blocks // group // batch, pick, 0)
    fetch.wait()
    chunk = min(MAP_BATCH, blocks // group)
    block_id = lax.broadcasted_iota(jnp.int32, (3 * group, cols), 0) % group

    def send(step, carry):
        for q in range(chunk):
            start = pl.multiple_of((step * chunk + q) * group, group)
            read = reads[pl.ds(3 * start, 3 * group), :]
            for k in range(0, group, 2):
                halves = [jnp.where(block_id == k + h, read, 0.0).astype(jnp.bfloat16) for h in range(2)]
                matrix = map_ref[pl.ds(start + k, 2)].reshape(2 * cols, cols)
                mapped = jnp.dot(
                    jnp.concatenate(halves, axis=1), matrix, preferred_element_type=jnp.float32
                )
                for h in range(2):
                    place = slot_ref[start + k + h] * slot_rows
                    for c in range(3):
                        at_row = c * group + k + h
                        send_out[pl.ds(place + c, 1), :] = mapped[at_row : at_row + 1]
                    if first:
                        send_out[pl.ds(place + 3, 1), :] = target_ref[
                            pl.ds(start + k + h, 1), :
                        ].astype(jnp.float32)
        return carry

    lax.fori_loop(0, blocks // group // chunk, send, 0)


def scatter_kernel(arrived_ref, *refs, first, last, sizes, batch):
    rows, cols, slots = sizes
    refs = list(refs)
    flag_ref = None if last else refs.pop(0)
    cells_ref = None if first else refs.pop(0)
    field_ref = None if last else refs.pop(0)
    applied_out = refs.pop(0)
    slot_rows = SLOT_ROWS if first else SLOT_ROWS - 1
    if first:
        cells_out = refs.pop(0)
        cells_out[...] = arrived_ref[pl.ds(SLOT_ROWS - 1, slots, stride=SLOT_ROWS), :].astype(jnp.int32)
        cells_ref = cells_out
    row_id = lax.broadcasted_iota(jnp.int32, (rows, cols), 0)
    col_id = lax.broadcasted_iota(jnp.int32, (cols, cols), 0)
    group = 8

    def add(step, total):
        spread, choose = [], []
        for part in range(batch // group):
            slot = pl.multiple_of(step * batch + part * group, group)
            cell = cells_ref[pl.ds(slot, group), :]
            cell_row, cell_col = cell // cols, cell % cols
            tile = arrived_ref[pl.ds(pl.multiple_of(slot * slot_rows, 8), group * slot_rows), :]
            for q in range(group):
                at = q * slot_rows
                here = row_id == cell_row[q : q + 1]
                spread.append(
                    jnp.concatenate(
                        [jnp.where(here, tile[at + c : at + c + 1], 0.0) for c in range(3)], axis=0
                    ).astype(jnp.bfloat16)
                )
                choose.append(
                    jnp.where(col_id == cell_col[q : q + 1], 1.0, 0.0).astype(jnp.bfloat16)
                )
        return total + lax.dot_general(
            jnp.concatenate(spread, axis=1),
            jnp.concatenate(choose, axis=1),
            (((1,), (1,)), ((), ())),
            preferred_element_type=jnp.float32,
        )

    total = lax.fori_loop(0, slots // batch, add, jnp.zeros((3 * rows, cols), jnp.float32))
    parts = [total[rows * c : rows * (c + 1)] for c in range(3)]
    for c in range(3):
        applied_out[c] = parts[c]
    if not last:
        pack_sides([field_ref[c] for c in range(3)] + parts, flag_ref, *refs)


def body(
    fields,
    coefficients,
    forcing,
    element_matrix,
    source_cells,
    target_cells,
    peer_map,
    mapping_blocks,
):
    rows_x, rows_y = lax.axis_size("gx"), lax.axis_size("gy")
    state, coef, force = fields[0], coefficients[0], forcing[0]
    comps, rows, cols = state.shape
    blocks = peer_map.shape[1]
    partners = rows_x * rows_y
    slots = partners * CAPACITY
    tall, wide = rows + 2 * HALO, 2 * cols
    place_x, place_y = lax.axis_index("gx"), lax.axis_index("gy")
    place = jnp.pad(
        jnp.stack([lax.axis_index("grp"), place_x, place_y]).astype(jnp.int32), (0, SCALARS - 3)
    )
    upper = lax.broadcasted_iota(jnp.int32, (16, cols), 0) < 8
    flags = jnp.where(upper, place_x % 2, place_y % 2).astype(jnp.int32)
    elements = jnp.pad(element_matrix.reshape(-1), (0, 2 * SCALARS - 144))
    full = pltpu.VMEM((comps, rows, cols), jnp.float32)
    full_hbm = jax.ShapeDtypeStruct((comps, rows, cols), jnp.float32)
    kept = pltpu.VMEM((5, tall, wide), jnp.float32)
    grp_swap = [(0, 1), (1, 0)]

    flags, *packed = pl.pallas_call(
        first_pack_kernel,
        out_shape=[pltpu.VMEM(flags.shape, jnp.int32)] + pack_shapes(7, rows, cols),
        name="first_pack",
        interpret=INTERPRET,
    )(flags, coef, force, state)
    slot_of, source, target = pl.pallas_call(
        prepare_kernel,
        out_shape=[
            jax.ShapeDtypeStruct((SCALARS,), jnp.int32),
            pltpu.VMEM((blocks, cols), jnp.int32),
            pltpu.VMEM((blocks, cols), jnp.int32),
        ],
        in_specs=[SMEM_SPEC] + [ANY_SPEC] * 2,
        out_specs=[SMEM_SPEC, VMEM_SPEC, VMEM_SPEC],
        scratch_shapes=[pltpu.SMEM((partners,), jnp.int32), pltpu.SemaphoreType.DMA((2,))],
        name="prepare",
        interpret=INTERPRET,
    )(peer_map[0, :, 0], source_cells[0], target_cells[0])
    applied, static, cells = None, None, None
    for outer in range(ITERS):
        first, last = outer == 0, outer == ITERS - 1
        sides = exchange(packed, flags)
        slot_rows = SLOT_ROWS if first else SLOT_ROWS - 1
        wire = pltpu.VMEM((slots * slot_rows, cols), jnp.float32)
        lead = (coef, force, state) if first else (static, state, applied)
        swept = pl.pallas_call(
            lambda *refs, first=first: sweep_kernel(
                *refs, first=first, sizes=(rows, cols, blocks), count_x=rows_x, count_y=rows_y
            ),
            out_shape=[full_hbm if last else full, wire] + ([kept] if first else []),
            in_specs=[ANY_SPEC] * 3 + [VMEM_SPEC] * 9 + [ANY_SPEC] + [VMEM_SPEC] * first,
            scratch_shapes=[
                pltpu.VMEM((7 if first else 6, tall, wide), jnp.float32),
                pltpu.VMEM((tall, cols), jnp.float32),
                pltpu.VMEM((tall, cols), jnp.float32),
                pltpu.VMEM((18, tall, wide), jnp.float32),
                pltpu.VMEM((blocks * 3, cols), jnp.float32),
                pltpu.VMEM(mapping_blocks.shape[1:], jnp.bfloat16),
                pltpu.SMEM((SCALARS,), jnp.int32),
                pltpu.SMEM((SCALARS,), jnp.int32),
                pltpu.SMEM((2 * SCALARS,), jnp.float32),
                pltpu.SemaphoreType.DMA((4,)),
            ],
            name="sweep_first" if first else "sweep",
            interpret=INTERPRET,
        )(
            place,
            slot_of,
            elements,
            near(flags),
            *(lead if first else map(near, lead)),
            *map(near, sides),
            near(source),
            mapping_blocks[0],
            *([near(target)] if first else []),
        )
        if first:
            state, send, static = swept
        else:
            state, send = swept
        crossed = lax.ppermute(send, "grp", grp_swap)
        arrived = lax.all_to_all(
            crossed.reshape((partners, CAPACITY * SLOT_ROWS, cols) if first else (partners, 3, CAPACITY, cols)),
            ("gx", "gy"),
            split_axis=0,
            concat_axis=0,
            tiled=True,
        ).reshape(slots * slot_rows, cols)
        received = pl.pallas_call(
            lambda *refs, first=first, last=last: scatter_kernel(
                *refs, first=first, last=last, sizes=(rows, cols, slots), batch=min(SCATTER_BATCH, slots)
            ),
            out_shape=[full_hbm if last else full]
            + ([pltpu.VMEM((slots, cols), jnp.int32)] if first else [])
            + ([] if last else pack_shapes(6, rows, cols)),
            name="scatter_first" if first else "scatter_last" if last else "scatter",
            interpret=INTERPRET,
        )(
            near(arrived),
            *([] if last else [near(flags)]),
            *([] if first else [near(cells)]),
            *([] if last else [near(state)]),
        )
        applied, packed = received[0], received[1:]
        if first:
            cells, packed = packed[0], packed[1:]
    return (state[None], applied[None])


def solution(mesh):
    placed = (
        P("grp", None, "gx", "gy"),
        P("grp", "gx", "gy"),
        P("grp", None, "gx", "gy"),
        P(),
        P("grp", ("gx", "gy"), None),
        P("grp", ("gx", "gy"), None),
        P("grp", ("gx", "gy"), None),
        P("grp", ("gx", "gy"), None, None),
    )
    return jax.shard_map(
        body,
        mesh=mesh,
        in_specs=placed,
        out_specs=(P("grp", None, "gx", "gy"), P("grp", None, "gx", "gy")),
        check_vma=False,
    )
```
